768 devices in a mesh: lat: 12 (over z), lon: 64 (over y, x, core).
Axes of the slice: x: 4, y: 8, z: 12, core: 2. Of those that a mesh axis runs over, the one named last changes fastest.
Arguments:
- fields: float32 [96, 2880, 384], P('lat', 'lon'), may hold values from -6 to 6
- cutoff: int32 [96], P('lat'), may hold values from 1 to 1425, as said below
Outputs:
- filtered: float32 [96, 2880, 384], P('lat', 'lon')
The draws below stay inside these ranges and needn't reach their ends.
Inputs may be any that keep to these rules, and one draw needn't show every extreme that they name: cutoff[g] lies between 1 and 1 + (1439)(2 p + 1) // 96, where p is the number of rows between row g and the nearer pole; this ceiling grows from the pole rows to the equator.
All inputs are finite; a program needn't handle non-finite values.
Results may differ from the reference program's by a relative error of at most 0.0003.
Values sent between devices are 32-bit elements; how exact they have to be, the bound alone decides.
A program may use at most 64 MiB of HBM per device.

```python
import jax
import jax.numpy as jnp
from jax import lax

NLON = 2880
FIELDS = 6
LEVELS = 64
NLAT = 96


def draw_cutoff(key, part):
    row_id = jnp.arange(NLAT, dtype=jnp.int32)
    pole_rows = jnp.minimum(row_id, NLAT - 1 - row_id)
    highest_cut = 1 + (NLON // 2 - 1) * (2 * pole_rows + 1) // NLAT
    drawn = jax.random.randint(key, (NLAT,), 1, highest_cut + 1, dtype=jnp.int32)
    drawn = drawn.at[NLAT // 2].set(highest_cut[NLAT // 2])
    drawn = drawn.at[NLAT - 1].set(1)
    return drawn


def block_levels(key, dims, split, smallest, top_value):
    level = 1.0
    for dim, shards_of in split:
        draws = jax.random.uniform(jax.random.fold_in(jax.random.fold_in(key, 6), dim), (shards_of,), jnp.float32, smallest / len(split), top_value / len(split))
        level = level * jnp.repeat(jnp.exp(draws), dims[dim] // shards_of).reshape((-1,) + (1,) * (len(dims) - 1 - dim))
    return level


def scatter_about(own_key, shape, scale, limit, split=(), kind=jnp.bfloat16):
    gain = block_levels(own_key, shape, split, -0.22, 0.18) if split else 1.0
    array = jax.random.normal(own_key, shape, jnp.float32) * scale * gain
    return jnp.minimum(jnp.maximum(array, -limit), limit).astype(kind)


def setup_inputs(seed: int = 0) -> dict:
    streams_of = jax.random.split(jax.random.key(seed), 3)
    fields = scatter_about(streams_of[0], (NLAT, NLON, FIELDS * LEVELS), 1.0, 6.0, ((0, 12), (1, 64)), jnp.float32)
    cutoff = draw_cutoff(jax.random.fold_in(streams_of[2], 71), 0)
    return {"fields": fields, "cutoff": cutoff}


def polar_mask(total_rows):
    latitude_row = jnp.arange(total_rows, dtype=jnp.int32)
    offset_twice = jnp.abs(2 * latitude_row + 1 - total_rows)
    return offset_twice * 5 > 2 * total_rows


def damping_row(cutoff_row, length):
    wavenumber = jnp.arange(length // 2 + 1, dtype=jnp.int32)
    cutoff_float = cutoff_row.astype(jnp.float32)
    wave_float = jnp.maximum(wavenumber, 1).astype(jnp.float32)
    ratio_value = jnp.sin(jnp.pi * cutoff_float / length) / jnp.sin(jnp.pi * wave_float / length)
    return jnp.where(wavenumber <= cutoff_row, 1.0, ratio_value * ratio_value).astype(jnp.float32)


def reference(fields, cutoff):
    total_rows = fields.shape[0]
    length = fields.shape[1]
    polar_rows = polar_mask(total_rows)

    def filter_row(packed):
        row_field, row_cutoff, row_polar = packed
        spectrum = jnp.fft.rfft(row_field, axis=0)
        scaled = spectrum * damping_row(row_cutoff, length)[:, None]
        smoothed = jnp.fft.irfft(scaled, n=length, axis=0).astype(jnp.float32)
        return jnp.where(row_polar, smoothed, row_field)

    return lax.map(filter_row, (fields, cutoff, polar_rows))
```

```python
import functools
import math

import jax
import jax.numpy as jnp
import numpy as np
from jax import lax
from jax.experimental import pallas as pl
from jax.experimental.pallas import tpu as pltpu
from jax.sharding import PartitionSpec as P

MESH = pl.DeviceIdType.MESH
F32 = jnp.float32
BF16 = jnp.bfloat16
NLON = 2880
SEG = 45
PAD = 48
ROWS = 8
LANES = 128
BLOCKS = 3
ORDER = (4, 3, 5, 2, 6, 1, 7)
HALF_ROOT = math.sqrt(0.5)


def base_waves():
    first = [0, 8, 16, 24, 4, 20, 36, 52, 32]
    return np.array([first] + [[q + 8 * p for p in range(8)] + [32] for q in (1, 2, 3)])


def make_tables():
    kappa = base_waves()
    span = np.arange(SEG)
    turn = 2.0 * np.pi * np.outer(span, span) / SEG
    base = np.zeros((2 * PAD, LANES))
    base[:SEG, :SEG] = np.cos(turn)
    base[PAD : PAD + SEG, :SEG] = np.sin(turn)
    rows = np.zeros((4, 32, LANES))
    columns = np.zeros((4, PAD, LANES))
    waves = np.zeros((4, PAD, LANES))
    for x in range(4):
        for p in range(9):
            angle = 2.0 * np.pi * kappa[x, p] * span / NLON
            rows[x, p, :SEG] = np.cos(angle)
            rows[x, 16 + p, :SEG] = np.sin(angle)
            columns[x, :SEG, p] = np.cos(angle)
            columns[x, :SEG, 16 + p] = np.sin(angle)
            wave = kappa[x, p] + 64 * span
            wave = np.minimum(wave, NLON - wave)
            waves[x, :SEG, p] = wave
            waves[x, :SEG, 16 + p] = 1.0 / np.sin(np.pi * np.maximum(wave, 1) / NLON) ** 2
    twist = np.zeros((4, 16))
    for x in range(4):
        for j in range(8):
            twist[x, j] = np.cos(2.0 * np.pi * x * j / 64)
            twist[x, 8 + j] = np.sin(2.0 * np.pi * x * j / 64)
    small = np.concatenate([rows, columns, waves], axis=1)
    return base.astype(np.float32), small.astype(np.float32), twist.astype(np.float32)


def real_dft(v):
    s = [v[i] + v[i + 4] for i in range(4)]
    d = [v[i] - v[i + 4] for i in range(4)]
    even, odd = s[0] + s[2], s[1] + s[3]
    minus = (d[1] - d[3]) * HALF_ROOT
    plus = (d[1] + d[3]) * HALF_ROOT
    return [
        (even + odd, even - odd),
        (d[0] + minus, -d[2] - plus),
        (s[0] - s[2], s[3] - s[1]),
        (d[0] - minus, d[2] - plus),
    ]


def real_idft(pairs):
    (a0, a4), (b_re, b_im), (c_re, c_im), (d_re, d_im) = pairs
    plus, minus = a0 + a4, a0 - a4
    c_re, c_im = c_re + c_re, c_im + c_im
    e = [plus + c_re, minus - c_im, plus - c_re, minus + c_im]
    diff = (b_re - d_re) * math.sqrt(2.0)
    both = (b_im + d_im) * math.sqrt(2.0)
    o = [2.0 * (b_re + d_re), diff - both, 2.0 * (d_im - b_im), -diff - both]
    return [e[i] + o[i] for i in range(4)] + [e[i] - o[i] for i in range(4)]


def turn_by(value, cos, sin):
    re, im = value
    return re * cos + im * sin, im * cos - re * sin


def add(a, b):
    return a[0] + b[0], a[1] + b[1]


def sub(a, b):
    return a[0] - b[0], a[1] - b[1]


def dft4(v):
    s02, d02, s13, d13 = add(v[0], v[2]), sub(v[0], v[2]), add(v[1], v[3]), sub(v[1], v[3])
    return [
        add(s02, s13),
        (d02[0] + d13[1], d02[1] - d13[0]),
        sub(s02, s13),
        (d02[0] - d13[1], d02[1] + d13[0]),
    ]


def idft4(v):
    s02, d02, s13, d13 = add(v[0], v[2]), sub(v[0], v[2]), add(v[1], v[3]), sub(v[1], v[3])
    return [
        add(s02, s13),
        (d02[0] - d13[1], d02[1] + d13[0]),
        sub(s02, s13),
        (d02[0] + d13[1], d02[1] - d13[0]),
    ]


def dft8(v):
    even = dft4([add(v[i], v[i + 4]) for i in range(4)])
    odd = [sub(v[i], v[i + 4]) for i in range(4)]
    odd = [
        odd[0],
        ((odd[1][0] + odd[1][1]) * HALF_ROOT, (odd[1][1] - odd[1][0]) * HALF_ROOT),
        (odd[2][1], -odd[2][0]),
        ((odd[3][1] - odd[3][0]) * HALF_ROOT, -(odd[3][0] + odd[3][1]) * HALF_ROOT),
    ]
    odd = dft4(odd)
    return [part[i] for i in range(4) for part in (even, odd)]


def idft8(v):
    even = idft4(v[0::2])
    odd = idft4(v[1::2])
    odd = [
        odd[0],
        ((odd[1][0] - odd[1][1]) * HALF_ROOT, (odd[1][1] + odd[1][0]) * HALF_ROOT),
        (-odd[2][1], odd[2][0]),
        (-(odd[3][0] + odd[3][1]) * HALF_ROOT, (odd[3][0] - odd[3][1]) * HALF_ROOT),
    ]
    return [add(even[i], odd[i]) for i in range(4)] + [sub(even[i], odd[i]) for i in range(4)]


SIXTEENTH = [(math.cos(math.pi * i / 8), math.sin(math.pi * i / 8)) for i in range(4)]


def first_chip_dft(z):
    low = real_dft([v[0] for v in z])
    turned = [turn_by((z[i][1], -z[i + 4][1]), *SIXTEENTH[i]) for i in range(4)]
    return low + dft4(turned)


def first_chip_idft(pairs):
    low = real_idft(pairs[:4])
    turned = idft4(pairs[4:])
    turned = [turn_by(turned[i], SIXTEENTH[i][0], -SIXTEENTH[i][1]) for i in range(4)]
    high = [2.0 * t[0] for t in turned] + [-2.0 * t[1] for t in turned]
    return list(zip(low, high))


def other_chip_dft(z, twist):
    return dft8([z[0]] + [turn_by(z[j], *twist[j]) for j in range(1, 8)])


def other_chip_idft(pairs, twist):
    z = idft8(pairs)
    return [z[0]] + [turn_by(z[j], twist[j][0], -twist[j][1]) for j in range(1, 8)]


def kernel(
    bands,
    cut_ref,
    twist_ref,
    x_hbm,
    base_hbm,
    small_hbm,
    out_hbm,
    xin,
    base,
    small,
    y_send,
    y_in,
    x_send,
    x_in,
    r_send,
    r_in,
    o_send,
    o_in,
    gate,
    high,
    low,
    result,
    load_sem,
    store_sem,
    ys_sem,
    yr_sem,
    xs_sem,
    xr_sem,
    rs_sem,
    rr_sem,
    os_sem,
    or_sem,
):
    band = lax.axis_index("lat")
    lon = lax.axis_index("lon")
    y, j = lon // 8, lon % 8
    x, core = j // 2, j % 2
    total_rows = bands * ROWS

    def polar(row):
        return jnp.abs(2 * (band * ROWS + row) + 1 - total_rows) * 5 > 2 * total_rows

    any_polar = polar(0) | polar(ROWS - 1)
    mine = polar(y)

    def keeper(b):
        return b if b < 2 else y % 2

    loads = [
        pltpu.make_async_copy(x_hbm.at[:, pl.ds(b * LANES, LANES)], xin.at[b], load_sem.at[b]) for b in range(BLOCKS)
    ]
    tables = [
        pltpu.make_async_copy(base_hbm, base, load_sem.at[3]),
        pltpu.make_async_copy(small_hbm.at[x], small, load_sem.at[4]),
    ]
    for copy in loads + tables:
        copy.start()

    barrier = pltpu.get_barrier_semaphore()

    @pl.when(any_polar)
    def _():
        for step in range(1, 8):
            there = (y + step) % 8
            pl.semaphore_signal(barrier, inc=1, device_id=(band, there * 8 + j), device_id_type=MESH)
            pl.semaphore_signal(barrier, inc=1, device_id=(band, y * 8 + (j + step) % 8), device_id_type=MESH)

    for copy in loads:
        copy.wait()

    def y_copy(b, there, sender):
        return pltpu.make_async_remote_copy(
            src_ref=y_send.at[b, there, pl.ds(0, SEG)],
            dst_ref=y_in.at[b, sender, pl.ds(0, SEG)],
            send_sem=ys_sem.at[b, there],
            recv_sem=yr_sem.at[b, sender],
            device_id=(band, there * 8 + j),
            device_id_type=MESH,
        )

    def x_copy(b, group, sender):
        return pltpu.make_async_remote_copy(
            src_ref=x_send.at[b, group, :, pl.ds(0, SEG)],
            dst_ref=x_in.at[b, sender, :, pl.ds(0, SEG)],
            send_sem=xs_sem.at[b, group],
            recv_sem=xr_sem.at[b, sender],
            device_id=(band, y * 8 + group * 2 + keeper(b)),
            device_id_type=MESH,
        )

    def r_copy(b, there, sender):
        return pltpu.make_async_remote_copy(
            src_ref=r_send.at[b, there, :, pl.ds(0, SEG)],
            dst_ref=r_in.at[b, sender, :, pl.ds(0, SEG)],
            send_sem=rs_sem.at[b, there],
            recv_sem=rr_sem.at[b, sender],
            device_id=(band, y * 8 + there),
            device_id_type=MESH,
        )

    def o_copy(b, there, sender):
        return pltpu.make_async_remote_copy(
            src_ref=o_send.at[b, there, pl.ds(0, SEG)],
            dst_ref=o_in.at[b, sender, pl.ds(0, SEG)],
            send_sem=os_sem.at[b, there],
            recv_sem=or_sem.at[b, sender],
            device_id=(band, there * 8 + j),
            device_id_type=MESH,
        )

    @pl.when(any_polar)
    def _():
        for b in range(BLOCKS):
            for row in range(ROWS):
                y_send[b, row, pl.ds(0, SEG), :] = xin[b, pl.ds(row, SEG, stride=ROWS), :]
        pl.semaphore_wait(barrier, 14)
        for b in range(BLOCKS):
            for step in ORDER:
                there = (y + step) % 8

                @pl.when(polar(there))
                def _():
                    y_copy(b, there, y).start()

    for copy in tables:
        copy.wait()

    def build_gates():
        cut = jnp.full((PAD, 1), cut_ref[y].astype(F32), F32)
        top = jnp.sin(cut * (math.pi / NLON))
        top = top * top
        cos_base, sin_base = base[0:PAD], base[PAD : 2 * PAD]

        def circulant(p):
            wave = small[32 + PAD : 32 + 2 * PAD, p : p + 1]
            inverse = small[32 + PAD : 32 + 2 * PAD, 16 + p : 17 + p]
            gain = jnp.where(wave <= cut, 1.0, top * inverse) * (1.0 / NLON)
            cos_row, sin_row = small[p : p + 1], small[16 + p : 17 + p]
            cos_col, sin_col = small[32 : 32 + PAD, p : p + 1], small[32 : 32 + PAD, 16 + p : 17 + p]
            cos_right = gain * (cos_base * cos_row - sin_base * sin_row)
            sin_right = gain * (sin_base * cos_row + cos_base * sin_row)
            cos_left = (cos_base * cos_col - sin_base * sin_col)[:, :PAD]
            sin_left = (sin_base * cos_col + cos_base * sin_col)[:, :PAD]
            dot = functools.partial(jnp.dot, precision=lax.Precision.HIGHEST, preferred_element_type=F32)
            real = dot(cos_left, cos_right) + dot(sin_left, sin_right)
            imag = dot(sin_left, cos_right) - dot(cos_left, sin_right)
            return real, imag

        def put(p, block):
            top_part = block.astype(BF16)
            gate[p, 0 : 2 * PAD] = top_part
            gate[p, 2 * PAD : 4 * PAD] = (block - top_part.astype(F32)).astype(BF16)

        for p in range(8):
            real, imag = circulant(p)
            lower = real
            if p == 0:
                second, _ = circulant(8)
                first = x == 0
                lower = jnp.where(first, second, real)
                imag = jnp.where(first, 0.0, imag)
            put(
                p,
                jnp.concatenate(
                    [real - pltpu.roll(imag, PAD, 1), imag + pltpu.roll(lower, PAD, 1)], axis=0
                ),
            )

    def y_stage(b):
        for step in ORDER:
            y_copy(b, y, (y + 8 - step) % 8).wait_recv()
        y_in[b, y, pl.ds(0, SEG)] = y_send[b, y, pl.ds(0, SEG)]
        for m in range(0, PAD, 16):
            rows = pl.ds(m, 16)
            pairs = real_dft([y_in[b, i, rows] for i in range(8)])
            for group in range(4):
                x_send[b, group, 0, rows], x_send[b, group, 1, rows] = pairs[group]
        for group in range(4):
            self_held = (x == group) & (core == keeper(b))

            @pl.when(self_held)
            def _():
                x_in[b, j, :, pl.ds(0, SEG)] = x_send[b, group, :, pl.ds(0, SEG)]

            @pl.when(jnp.logical_not(self_held))
            def _():
                x_copy(b, group, j).start()

    def x_stage(b):
        for step in range(1, 8):
            x_copy(b, x, (j + step) % 8).wait_recv()
        twist = [(twist_ref[x, i], twist_ref[x, 8 + i]) for i in range(8)]
        for m in range(0, PAD, 16):
            rows = pl.ds(m, 16)
            keep = lax.broadcasted_iota(jnp.int32, (16, LANES), 0) < SEG - m

            def take(i, c):
                value = x_in[b, i, c, rows]
                return value if m + 16 <= SEG else jnp.where(keep, value, 0.0)

            def write(pairs):
                for p in range(8):
                    for c in range(2):
                        value = pairs[p][c]
                        big = value.astype(BF16)
                        high[p, pl.ds(c * PAD + m, 16)] = big
                        low[p, pl.ds(c * PAD + m, 16)] = (value - big.astype(F32)).astype(BF16)

            @pl.when(x == 0)
            def _():
                write(first_chip_dft([(take(i, 0), take(i, 1)) for i in range(8)]))

            @pl.when(x != 0)
            def _():
                write(other_chip_dft([(take(i, 0), take(i, 1)) for i in range(8)], twist))

        for p in range(8):
            both = jnp.dot(gate[p, :, 0 : 2 * PAD], high[p], preferred_element_type=F32)
            rest = jnp.dot(gate[p, 0 : 2 * PAD, 0 : 2 * PAD], low[p], preferred_element_type=F32)
            result[p] = both[0 : 2 * PAD] + both[2 * PAD : 4 * PAD] + rest
        for m in range(0, PAD, 16):
            rows = pl.ds(m, 16)

            def pairs():
                return [(result[p, pl.ds(m, 16)], result[p, pl.ds(PAD + m, 16)]) for p in range(8)]

            def write_back(z):
                for i in range(8):
                    r_send[b, i, 0, rows], r_send[b, i, 1, rows] = z[i]

            @pl.when(x == 0)
            def _():
                write_back(first_chip_idft(pairs()))

            @pl.when(x != 0)
            def _():
                write_back(other_chip_idft(pairs(), twist))

        for step in range(1, 8):
            r_copy(b, (j + step) % 8, x).start()
        r_in[b, x, :, pl.ds(0, SEG)] = r_send[b, j, :, pl.ds(0, SEG)]

    def r_stage(b):
        for group in range(4):
            self_held = (x == group) & (core == keeper(b))

            @pl.when(jnp.logical_not(self_held))
            def _():
                r_copy(b, j, group).wait_recv()

        for m in range(0, PAD, 16):
            rows = pl.ds(m, 16)
            values = real_idft([(r_in[b, g, 0, rows], r_in[b, g, 1, rows]) for g in range(4)])
            for i in range(8):
                o_send[b, i, rows] = values[i]
        for step in ORDER:
            o_copy(b, (y + step) % 8, y).start()
        o_in[b, y, pl.ds(0, SEG)] = o_send[b, y, pl.ds(0, SEG)]

    def held_x_stage(b):
        @pl.when(core == keeper(b))
        def _():
            x_stage(b)

    @pl.when(mine)
    def _():
        build_gates()
        y_stage(0)
        y_stage(1)
        held_x_stage(0)
        y_stage(2)
        held_x_stage(1)
        r_stage(0)
        held_x_stage(2)
        r_stage(1)
        r_stage(2)

    stores = [
        pltpu.make_async_copy(xin.at[b], out_hbm.at[:, pl.ds(b * LANES, LANES)], store_sem.at[b])
        for b in range(BLOCKS)
    ]
    for b in range(BLOCKS):

        @pl.when(any_polar)
        def _():
            for step in ORDER:
                there = (y + 8 - step) % 8

                @pl.when(polar(there))
                def _():
                    o_copy(b, y, there).wait_recv()

            for row in range(ROWS):

                @pl.when(polar(row))
                def _():
                    xin[b, pl.ds(row, SEG, stride=ROWS), :] = o_in[b, row, pl.ds(0, SEG), :]

        stores[b].start()

    @pl.when(any_polar)
    def _():
        for b in range(BLOCKS):
            for step in ORDER:
                there = (y + step) % 8

                @pl.when(polar(there))
                def _():
                    y_copy(b, there, y).wait_send()

    @pl.when(mine)
    def _():
        for b in range(BLOCKS):
            for group in range(4):

                @pl.when(jnp.logical_not((x == group) & (core == keeper(b))))
                def _():
                    x_copy(b, group, j).wait_send()

            @pl.when(core == keeper(b))
            def _():
                for step in range(1, 8):
                    r_copy(b, (j + step) % 8, x).wait_send()

            for step in ORDER:
                o_copy(b, (y + step) % 8, y).wait_send()

    for copy in stores:
        copy.wait()


def local(bands, fields, cutoff):
    base, small, twist = make_tables()
    flat = jnp.transpose(fields, (1, 0, 2)).reshape(SEG * ROWS, BLOCKS * LANES)
    vmem, dma = pltpu.VMEM, pltpu.SemaphoreType.DMA
    any_space = pl.BlockSpec(memory_space=pl.ANY)
    smem = pl.BlockSpec(memory_space=pltpu.SMEM)
    out = pl.pallas_call(
        functools.partial(kernel, bands),
        out_shape=jax.ShapeDtypeStruct(flat.shape, F32),
        in_specs=[smem, smem, any_space, any_space, any_space],
        out_specs=any_space,
        scratch_shapes=[
            vmem((BLOCKS, SEG * ROWS, LANES), F32),
            vmem(base.shape, F32),
            vmem(small.shape[1:], F32),
            vmem((BLOCKS, 8, PAD, LANES), F32),
            vmem((BLOCKS, 8, PAD, LANES), F32),
            vmem((BLOCKS, 4, 2, PAD, LANES), F32),
            vmem((BLOCKS, 8, 2, PAD, LANES), F32),
            vmem((BLOCKS, 8, 2, PAD, LANES), F32),
            vmem((BLOCKS, 4, 2, PAD, LANES), F32),
            vmem((BLOCKS, 8, PAD, LANES), F32),
            vmem((BLOCKS, 8, PAD, LANES), F32),
            vmem((8, 4 * PAD, LANES), BF16),
            vmem((8, 2 * PAD, LANES), BF16),
            vmem((8, 2 * PAD, LANES), BF16),
            vmem((8, 2 * PAD, LANES), F32),
            dma((5,)),
            dma((BLOCKS,)),
            dma((BLOCKS, 8)),
            dma((BLOCKS, 8)),
            dma((BLOCKS, 4)),
            dma((BLOCKS, 8)),
            dma((BLOCKS, 8)),
            dma((BLOCKS, 4)),
            dma((BLOCKS, 8)),
            dma((BLOCKS, 8)),
        ],
        compiler_params=pltpu.CompilerParams(collective_id=0, has_side_effects=True),
    )(cutoff, jnp.asarray(twist), flat, jnp.asarray(base), jnp.asarray(small))
    return jnp.transpose(out.reshape(SEG, ROWS, BLOCKS * LANES), (1, 0, 2))


def solution(mesh):
    return jax.shard_map(
        functools.partial(local, mesh.shape["lat"]),
        mesh=mesh,
        in_specs=(P("lat", "lon", None), P("lat")),
        out_specs=P("lat", "lon", None),
        check_vma=False,
    )
```

```python
import functools
import math

import jax
import jax.numpy as jnp
from jax import lax
from jax.experimental import pallas as pl
from jax.experimental.pallas import tpu as pltpu
from jax.sharding import PartitionSpec as P

MESH = pl.DeviceIdType.MESH
F32 = jnp.float32
BF16 = jnp.bfloat16
NLON = 2880
SEG = 45
PAD = 48
HALF = 23
SLOT = 24
ROWS = 8
LANES = 128
BLOCKS = 3
CHUNKS = 6
ORDER = (4, 3, 5, 2, 6, 1, 7)
HUB = 4
X_LAG = 2
R_LAG = 4
HALF_ROOT = math.sqrt(0.5)


FIRST_WAVES = (0, 8, 16, 24, 4, 20, 36, 52, 32)
COS_TERMS = [(-1) ** i / math.factorial(2 * i) for i in range(11)]
SIN_TERMS = [(-1) ** i / math.factorial(2 * i + 1) for i in range(11)]


def cos_sin(angle):
    square = angle * angle
    cos, sin = COS_TERMS[-1], SIN_TERMS[-1]
    for i in reversed(range(10)):
        cos, sin = cos * square + COS_TERMS[i], sin * square + SIN_TERMS[i]
    return cos, sin * angle


def wave_at(step):
    step = step - NLON * jnp.floor(step * (1.0 / NLON) + 0.5)
    return cos_sin(step * (2.0 * math.pi / NLON))


def real_dft(v):
    s = [v[i] + v[i + 4] for i in range(4)]
    d = [v[i] - v[i + 4] for i in range(4)]
    even, odd = s[0] + s[2], s[1] + s[3]
    minus = (d[1] - d[3]) * HALF_ROOT
    plus = (d[1] + d[3]) * HALF_ROOT
    return [
        (even + odd, even - odd),
        (d[0] + minus, -d[2] - plus),
        (s[0] - s[2], s[3] - s[1]),
        (d[0] - minus, d[2] - plus),
    ]


def real_idft(pairs):
    (a0, a4), (b_re, b_im), (c_re, c_im), (d_re, d_im) = pairs
    plus, minus = a0 + a4, a0 - a4
    c_re, c_im = c_re + c_re, c_im + c_im
    e = [plus + c_re, minus - c_im, plus - c_re, minus + c_im]
    diff = (b_re - d_re) * math.sqrt(2.0)
    both = (b_im + d_im) * math.sqrt(2.0)
    o = [2.0 * (b_re + d_re), diff - both, 2.0 * (d_im - b_im), -diff - both]
    return [e[i] + o[i] for i in range(4)] + [e[i] - o[i] for i in range(4)]


def turn_by(value, cos, sin):
    re, im = value
    return re * cos + im * sin, im * cos - re * sin


def add(a, b):
    return a[0] + b[0], a[1] + b[1]


def sub(a, b):
    return a[0] - b[0], a[1] - b[1]


def dft4(v):
    s02, d02, s13, d13 = add(v[0], v[2]), sub(v[0], v[2]), add(v[1], v[3]), sub(v[1], v[3])
    return [
        add(s02, s13),
        (d02[0] + d13[1], d02[1] - d13[0]),
        sub(s02, s13),
        (d02[0] - d13[1], d02[1] + d13[0]),
    ]


def idft4(v):
    s02, d02, s13, d13 = add(v[0], v[2]), sub(v[0], v[2]), add(v[1], v[3]), sub(v[1], v[3])
    return [
        add(s02, s13),
        (d02[0] - d13[1], d02[1] + d13[0]),
        sub(s02, s13),
        (d02[0] + d13[1], d02[1] - d13[0]),
    ]


def dft8(v):
    even = dft4([add(v[i], v[i + 4]) for i in range(4)])
    odd = [sub(v[i], v[i + 4]) for i in range(4)]
    odd = [
        odd[0],
        ((odd[1][0] + odd[1][1]) * HALF_ROOT, (odd[1][1] - odd[1][0]) * HALF_ROOT),
        (odd[2][1], -odd[2][0]),
        ((odd[3][1] - odd[3][0]) * HALF_ROOT, -(odd[3][0] + odd[3][1]) * HALF_ROOT),
    ]
    odd = dft4(odd)
    return [part[i] for i in range(4) for part in (even, odd)]


def idft8(v):
    even = idft4(v[0::2])
    odd = idft4(v[1::2])
    odd = [
        odd[0],
        ((odd[1][0] - odd[1][1]) * HALF_ROOT, (odd[1][1] + odd[1][0]) * HALF_ROOT),
        (-odd[2][1], odd[2][0]),
        (-(odd[3][0] + odd[3][1]) * HALF_ROOT, (odd[3][0] - odd[3][1]) * HALF_ROOT),
    ]
    return [add(even[i], odd[i]) for i in range(4)] + [sub(even[i], odd[i]) for i in range(4)]


SIXTEENTH = [(math.cos(math.pi * i / 8), math.sin(math.pi * i / 8)) for i in range(4)]


def first_chip_dft(z):
    low = real_dft([v[0] for v in z])
    turned = [turn_by((z[i][1], -z[i + 4][1]), *SIXTEENTH[i]) for i in range(4)]
    return low + dft4(turned)


def first_chip_idft(pairs):
    low = real_idft(pairs[:4])
    turned = idft4(pairs[4:])
    turned = [turn_by(turned[i], SIXTEENTH[i][0], -SIXTEENTH[i][1]) for i in range(4)]
    high = [2.0 * t[0] for t in turned] + [-2.0 * t[1] for t in turned]
    return list(zip(low, high))


def other_chip_dft(z, twist):
    return dft8([z[0]] + [turn_by(z[j], *twist[j]) for j in range(1, 8)])


def other_chip_idft(pairs, twist):
    z = idft8(pairs)
    return [z[0]] + [turn_by(z[j], twist[j][0], -twist[j][1]) for j in range(1, 8)]


def kernel(
    bands,
    cut_hbm,
    x_hbm,
    out,
    cut_ref,
    twist_ref,
    y_send,
    y_in,
    x_send,
    x_in,
    r_send,
    r_in,
    o_send,
    o_in,
    gate,
    stage,
    result,
    load_sem,
    ys_sem,
    yr_sem,
    xs_sem,
    xr_sem,
    rs_sem,
    rr_sem,
    os_sem,
    or_sem,
    meet_sem,
    go_sem,
):
    band = lax.axis_index("lat")
    lon = lax.axis_index("lon")
    y, j = lon // 8, lon % 8
    x, core = j // 2, j % 2
    total_rows = bands * ROWS

    def polar(row):
        return jnp.abs(2 * (band * ROWS + row) + 1 - total_rows) * 5 > 2 * total_rows

    count = sum(polar(row).astype(jnp.int32) for row in range(ROWS))
    first = jnp.where(polar(0), 0, ROWS - count)
    any_polar = count > 0

    def place(there):
        index = (there * count + 7) // 8
        return index, (index < count) & (index * 8 // jnp.maximum(count, 1) == there)

    index, mine = place(y)
    mine = mine & any_polar
    row_here = jnp.minimum(first + index, ROWS - 1)

    def keeper(c):
        return c % 2

    load = pltpu.make_async_copy(x_hbm, out, load_sem.at[0])
    cut_load = pltpu.make_async_copy(cut_hbm, cut_ref, load_sem.at[1])
    load.start()

    barrier = pltpu.get_barrier_semaphore()

    @pl.when(any_polar)
    def _():
        for step in ORDER:
            pl.semaphore_signal(barrier, inc=1, device_id=(band, (y + step) % 8 * 8 + j), device_id_type=MESH)

        @pl.when(y == HUB)
        def _():
            for step in range(1, 8):
                pl.semaphore_signal(barrier, inc=1, device_id=(band, y * 8 + (j + step) % 8), device_id_type=MESH)

    cut_load.start()
    load.wait()

    def y_copy(c, there, row, sender):
        return pltpu.make_async_remote_copy(
            src_ref=y_send.at[c, row, pl.ds(0, HALF)],
            dst_ref=y_in.at[c, sender, pl.ds(0, HALF)],
            send_sem=ys_sem,
            recv_sem=yr_sem.at[c],
            device_id=(band, there * 8 + j),
            device_id_type=MESH,
        )

    def x_copy(c, group, sender):
        return pltpu.make_async_remote_copy(
            src_ref=x_send.at[c, group, :, pl.ds(0, HALF)],
            dst_ref=x_in.at[c, sender, :, pl.ds(0, HALF)],
            send_sem=xs_sem.at[(core == keeper(c)).astype(jnp.int32)],
            recv_sem=xr_sem.at[c],
            device_id=(band, y * 8 + group * 2 + keeper(c)),
            device_id_type=MESH,
        )

    def r_copy(c, there, sender):
        return pltpu.make_async_remote_copy(
            src_ref=r_send.at[c, there, :, pl.ds(0, HALF)],
            dst_ref=r_in.at[c, sender, :, pl.ds(0, HALF)],
            send_sem=rs_sem,
            recv_sem=rr_sem.at[c],
            device_id=(band, y * 8 + there),
            device_id_type=MESH,
        )

    def o_copy(c, there, row, sender):
        return pltpu.make_async_remote_copy(
            src_ref=o_send.at[c, there, pl.ds(0, HALF)],
            dst_ref=o_in.at[c, row, pl.ds(0, HALF)],
            send_sem=os_sem,
            recv_sem=or_sem.at[c],
            device_id=(band, there * 8 + j),
            device_id_type=MESH,
        )

    def await_bytes(ref, sem):
        pltpu.make_async_copy(ref, ref, sem).wait()

    def await_parts(ref_of, sem, parts, choices):
        for choice in choices:

            @pl.when(parts == choice)
            def _():
                await_bytes(ref_of(choice), sem)

    rows_used = pl.ds(0, HALF)
    others = count - mine.astype(jnp.int32)

    low_lanes = lax.broadcasted_iota(jnp.int32, (HALF, LANES), 1) < 64

    def swap(value):
        return pltpu.roll(value, 64, 1)

    @pl.when(any_polar)
    def _():
        @pl.loop(0, ROWS)
        def _(row):
            for b in range(BLOCKS):
                upper = out[pl.ds(b * ROWS + row, HALF, stride=BLOCKS * ROWS), :]
                lower = out[pl.ds((HALF - 1) * BLOCKS * ROWS + b * ROWS + row, HALF, stride=BLOCKS * ROWS), :]
                y_send[2 * b, row, pl.ds(0, HALF), :] = jnp.where(low_lanes, upper, swap(lower))
                y_send[2 * b + 1, row, pl.ds(0, HALF), :] = jnp.where(low_lanes, swap(upper), lower)

        @pl.when(y == HUB)
        def _():
            pl.semaphore_wait(barrier, 14)
            for step in range(1, 8):
                pl.semaphore_signal(meet_sem, inc=1, device_id=(band, y * 8 + (j + step) % 8), device_id_type=MESH)

        @pl.when(y != HUB)
        def _():
            pl.semaphore_wait(barrier, 7)

        @pl.loop(0, CHUNKS)
        def _(c):
            for step in ORDER:
                there = (y + step) % 8
                index_there, holds = place(there)

                @pl.when(holds)
                def _():
                    y_copy(c, there, first + index_there, y).start()

        @pl.when(y == HUB)
        def _():
            pl.semaphore_wait(meet_sem, 7)
            for step in ORDER:
                pl.semaphore_signal(go_sem, inc=1, device_id=(band, (y + step) % 8 * 8 + j), device_id_type=MESH)

    cut_load.wait()

    def build_gates():
        shape = (PAD, LANES)
        down = lax.broadcasted_iota(jnp.int32, shape, 0)
        across = lax.broadcasted_iota(jnp.int32, shape, 1)

        def longitude(slot):
            return jnp.where(slot < SLOT, slot, slot - SLOT + HALF - 1).astype(F32)

        slot = jnp.where(across < 64, across, jnp.where(across < 64 + SLOT, across - 64 + SLOT, across - 64 - SLOT))
        valid = (slot != HALF) & (slot != SLOT) & (slot < PAD - 1) & (slot >= 0)
        valid = valid & (down < SEG) & ((across < PAD) | ((across >= 64) & (across < 64 + PAD)))
        m_across, m_down = longitude(slot), longitude(down)
        valid_left = (down != HALF) & (down != PAD - 1) & (across < SEG)
        k_down, k_across = 64.0 * down.astype(F32), 64.0 * across.astype(F32)
        upper_rows, used = down < SLOT, across < PAD
        cut = jnp.full(shape, cut_ref[row_here].astype(F32), F32)
        top = cos_sin(cut * (math.pi / NLON))[1]
        rows = lax.broadcasted_iota(jnp.int32, (8, LANES), 0)
        twist_ref[0:8], twist_ref[8:16] = wave_at((rows * x * SEG).astype(F32))

        def ordered(block):
            return jnp.where(used, jnp.where(upper_rows, block, swap(block)), 0.0)

        def circulant(p, base):
            wave = base + k_down
            cos_right, sin_right = wave_at(wave * m_across)
            folded = jnp.minimum(wave, NLON - wave)
            ratio = top / cos_sin(jnp.maximum(folded, 1.0) * (math.pi / NLON))[1]
            gain = jnp.where(valid, jnp.where(folded <= cut, 1.0, ratio * ratio) * (1.0 / NLON), 0.0)
            cos_right, sin_right = gain * cos_right, gain * sin_right
            cos_left, sin_left = wave_at((base + k_across) * m_down)
            cos_left = jnp.where(valid_left, cos_left, 0.0)[:, :PAD]
            sin_left = jnp.where(valid_left, sin_left, 0.0)[:, :PAD]
            dot = functools.partial(jnp.dot, precision=lax.Precision.HIGHEST, preferred_element_type=F32)
            real = dot(cos_left, cos_right) + dot(sin_left, sin_right)
            imag = dot(sin_left, cos_right) - dot(cos_left, sin_right)
            return ordered(real), ordered(imag)

        def put(p, real, lower, imag):
            block = jnp.concatenate(
                [real - pltpu.roll(imag, PAD, 1), imag + pltpu.roll(lower, PAD, 1)], axis=0
            )
            top_part = block.astype(BF16)
            gate[p, 0 : 2 * PAD] = top_part
            gate[p, 2 * PAD : 4 * PAD] = (block - top_part.astype(F32)).astype(BF16)

        @pl.loop(0, 8)
        def _(p):
            base = x + 8 * p
            for i in range(8):
                base = jnp.where((x == 0) & (p == i), FIRST_WAVES[i], base)
            real, imag = circulant(p, base.astype(F32))
            put(p, real, real, imag)

        @pl.when(x == 0)
        def _():
            put(0, circulant(0, 0.0)[0], circulant(0, float(FIRST_WAVES[8]))[0], jnp.zeros(shape, F32))

    def y_stage(c):
        await_bytes(y_in.at[c, pl.ds(0, 7), rows_used], yr_sem.at[c])
        y_in[c, y, pl.ds(0, HALF)] = y_send[c, row_here, pl.ds(0, HALF)]
        @pl.loop(0, SLOT, step=8)
        def _(m):
            rows = pl.ds(pl.multiple_of(m, 8), 8)
            pairs = real_dft([y_in[c, i, rows] for i in range(8)])
            for group in range(4):
                x_send[c, group, 0, rows], x_send[c, group, 1, rows] = pairs[group]

        @pl.when((c == 0) & (y != HUB))
        def _():
            pl.semaphore_wait(go_sem, 1)

        for group in range(4):
            self_held = (x == group) & (core == keeper(c))

            @pl.when(self_held)
            def _():
                x_in[c, j, :, pl.ds(0, HALF)] = x_send[c, group, :, pl.ds(0, HALF)]

            @pl.when(jnp.logical_not(self_held))
            def _():
                x_copy(c, group, j).start()

    def x_stage(c):
        await_bytes(x_in.at[c, pl.ds(0, 7), :, rows_used], xr_sem.at[c])
        twist = [(twist_ref[i : i + 1], twist_ref[8 + i : 9 + i]) for i in range(8)]
        eight = lax.broadcasted_iota(jnp.int32, (8, LANES), 0)
        low_eight = lax.broadcasted_iota(jnp.int32, (8, LANES), 1) < 64

        def take(i, part, m):
            return jnp.where(eight < HALF - m, x_in[c, i, part, pl.ds(m, 8)], 0.0)

        def write(pairs, m):
            for p in range(8):
                for part in range(2):
                    stage[p, pl.ds(part * PAD + m, 8)] = pairs[p][part]
                    stage[p, pl.ds(part * PAD + SLOT + m, 8)] = swap(pairs[p][part])

        @pl.when(x == 0)
        def _():
            @pl.loop(0, SLOT, step=8)
            def _(m):
                m = pl.multiple_of(m, 8)
                write(first_chip_dft([(take(i, 0, m), take(i, 1, m)) for i in range(8)]), m)

        @pl.when(x != 0)
        def _():
            @pl.loop(0, SLOT, step=8)
            def _(m):
                m = pl.multiple_of(m, 8)
                write(other_chip_dft([(take(i, 0, m), take(i, 1, m)) for i in range(8)], twist), m)

        for p in range(8):
            value = stage[p]
            big = value.astype(BF16)
            small_part = (value - big.astype(F32)).astype(BF16)
            both = jnp.dot(gate[p, :, 0 : 2 * PAD], big, preferred_element_type=F32)
            rest = jnp.dot(gate[p, 0 : 2 * PAD, 0 : 2 * PAD], small_part, preferred_element_type=F32)
            result[p] = both[0 : 2 * PAD] + both[2 * PAD : 4 * PAD] + rest

        def pairs_at(m):
            def pick(p, part):
                return jnp.where(
                    low_eight, result[p, pl.ds(part * PAD + m, 8)], result[p, pl.ds(part * PAD + SLOT + m, 8)]
                )

            return [(pick(p, 0), pick(p, 1)) for p in range(8)]

        def write_back(z, m):
            for i in range(8):
                r_send[c, i, 0, pl.ds(m, 8)], r_send[c, i, 1, pl.ds(m, 8)] = z[i]

        @pl.when(x == 0)
        def _():
            @pl.loop(0, SLOT, step=8)
            def _(m):
                m = pl.multiple_of(m, 8)
                write_back(first_chip_idft(pairs_at(m)), m)

        @pl.when(x != 0)
        def _():
            @pl.loop(0, SLOT, step=8)
            def _(m):
                m = pl.multiple_of(m, 8)
                write_back(other_chip_idft(pairs_at(m), twist), m)

        for step in (4, 5, 3, 2, 6, 7, 1):
            r_copy(c, (j + step) % 8, x).start()
        r_in[c, x, :, pl.ds(0, HALF)] = r_send[c, j, :, pl.ds(0, HALF)]

    def r_stage(c):
        await_parts(
            lambda n: r_in.at[c, pl.ds(0, n), :, rows_used],
            rr_sem.at[c],
            4 - (core == keeper(c)).astype(jnp.int32),
            (3, 4),
        )

        @pl.loop(0, SLOT, step=8)
        def _(m):
            rows = pl.ds(pl.multiple_of(m, 8), 8)
            values = real_idft([(r_in[c, g, 0, rows], r_in[c, g, 1, rows]) for g in range(4)])
            for i in range(8):
                o_send[c, i, rows] = values[i]
        for step in ORDER:
            o_copy(c, (y + step) % 8, row_here, y).start()
        o_in[c, row_here, pl.ds(0, HALF)] = o_send[c, y, pl.ds(0, HALF)]

    @pl.when(mine)
    def _():
        build_gates()

        @pl.loop(0, CHUNKS + R_LAG)
        def _(t):
            @pl.when(t < CHUNKS)
            def _():
                y_stage(t)

            @pl.when((t >= X_LAG) & (t < CHUNKS + X_LAG) & (core == keeper(t - X_LAG)))
            def _():
                x_stage(t - X_LAG)

            @pl.when(t >= R_LAG)
            def _():
                r_stage(t - R_LAG)

    @pl.when(any_polar & jnp.logical_not(mine) & (y != HUB))
    def _():
        pl.semaphore_wait(go_sem, 1)

    @pl.when(any_polar)
    def _():
        @pl.loop(0, BLOCKS)
        def _(b):
            for c in (2 * b, 2 * b + 1):
                await_parts(lambda n: o_in.at[c, pl.ds(0, n), rows_used], or_sem.at[c], others, range(1, 8))

            @pl.loop(0, ROWS)
            def _(row):
                @pl.when(polar(row))
                def _():
                    left, right = o_in[2 * b, row, pl.ds(0, HALF), :], o_in[2 * b + 1, row, pl.ds(0, HALF), :]
                    start = b * ROWS + row
                    out[pl.ds(start, HALF, stride=BLOCKS * ROWS), :] = jnp.where(low_lanes, left, swap(right))
                    out[pl.ds((HALF - 1) * BLOCKS * ROWS + start, HALF, stride=BLOCKS * ROWS), :] = jnp.where(
                        low_lanes, swap(left), right
                    )

        await_parts(lambda n: y_send.at[:, pl.ds(0, n), rows_used], ys_sem, others, range(1, 8))

    @pl.when(mine)
    def _():
        await_bytes(x_send.at[pl.ds(0, CHUNKS // 2), :, :, rows_used], xs_sem.at[0])
        await_bytes(x_send.at[pl.ds(0, CHUNKS // 2), pl.ds(0, 3), :, rows_used], xs_sem.at[1])
        await_bytes(r_send.at[pl.ds(0, CHUNKS // 2), pl.ds(0, 7), :, rows_used], rs_sem)
        await_bytes(o_send.at[:, pl.ds(0, 7), rows_used], os_sem)


def local(bands, fields, cutoff):
    flat = jnp.transpose(fields.reshape(ROWS, SEG, BLOCKS, LANES), (1, 2, 0, 3)).reshape(SEG * BLOCKS * ROWS, LANES)
    vmem, dma = pltpu.VMEM, pltpu.SemaphoreType.DMA
    hbm = pl.BlockSpec(memory_space=pltpu.HBM)
    out = pl.pallas_call(
        functools.partial(kernel, bands),
        out_shape=jax.ShapeDtypeStruct(flat.shape, F32),
        in_specs=[hbm] * 2,
        out_specs=pl.BlockSpec(memory_space=pltpu.VMEM),
        scratch_shapes=[
            pltpu.SMEM((ROWS,), jnp.int32),
            vmem((16, LANES), F32),
            vmem((CHUNKS, 8, SLOT, LANES), F32),
            vmem((CHUNKS, 8, SLOT, LANES), F32),
            vmem((CHUNKS, 4, 2, SLOT, LANES), F32),
            vmem((CHUNKS, 8, 2, SLOT, LANES), F32),
            vmem((CHUNKS, 8, 2, SLOT, LANES), F32),
            vmem((CHUNKS, 4, 2, SLOT, LANES), F32),
            vmem((CHUNKS, 8, SLOT, LANES), F32),
            vmem((CHUNKS, 8, SLOT, LANES), F32),
            vmem((8, 4 * PAD, LANES), BF16),
            vmem((8, 2 * PAD, LANES), F32),
            vmem((8, 2 * PAD, LANES), F32),
            dma((2,)),
            dma,
            dma((CHUNKS,)),
            dma((2,)),
            dma((CHUNKS,)),
            dma,
            dma((CHUNKS,)),
            dma,
            dma((CHUNKS,)),
            pltpu.SemaphoreType.REGULAR,
            pltpu.SemaphoreType.REGULAR,
        ],
        compiler_params=pltpu.CompilerParams(
            collective_id=0, has_side_effects=True, vmem_limit_bytes=54304 * 1024
        ),
    )(cutoff, flat)
    filtered = jnp.transpose(out.reshape(SEG, BLOCKS, ROWS, LANES), (2, 0, 1, 3))
    return filtered.reshape(ROWS, SEG, BLOCKS * LANES)


def solution(mesh):
    return jax.shard_map(
        functools.partial(local, mesh.shape["lat"]),
        mesh=mesh,
        in_specs=(P("lat", "lon", None), P("lat")),
        out_specs=P("lat", "lon", None),
        check_vma=False,
    )
```

```python
import functools
import math

import jax
import jax.numpy as jnp
from jax import lax
from jax.experimental import pallas as pl
from jax.experimental.pallas import tpu as pltpu
from jax.sharding import PartitionSpec as P

MESH = pl.DeviceIdType.MESH
F32 = jnp.float32
BF16 = jnp.bfloat16
NLON = 2880
SEG = 45
PAD = 48
HALF = 23
SLOT = 24
ROWS = 8
LANES = 128
BLOCKS = 3
CHUNKS = 6
ORDER = (4, 3, 5, 2, 6, 1, 7)
HUB = 1
HALF_ROOT = math.sqrt(0.5)


FIRST_WAVES = (0, 8, 16, 24, 4, 20, 36, 52, 32)
COS_TERMS = [(-1) ** i / math.factorial(2 * i) for i in range(11)]
SIN_TERMS = [(-1) ** i / math.factorial(2 * i + 1) for i in range(11)]


def cos_sin(angle):
    square = angle * angle
    cos, sin = COS_TERMS[-1], SIN_TERMS[-1]
    for i in reversed(range(10)):
        cos, sin = cos * square + COS_TERMS[i], sin * square + SIN_TERMS[i]
    return cos, sin * angle


def wave_at(step):
    step = step - NLON * jnp.floor(step * (1.0 / NLON) + 0.5)
    return cos_sin(step * (2.0 * math.pi / NLON))


def real_dft(v):
    s = [v[i] + v[i + 4] for i in range(4)]
    d = [v[i] - v[i + 4] for i in range(4)]
    even, odd = s[0] + s[2], s[1] + s[3]
    minus = (d[1] - d[3]) * HALF_ROOT
    plus = (d[1] + d[3]) * HALF_ROOT
    return [
        (even + odd, even - odd),
        (d[0] + minus, -d[2] - plus),
        (s[0] - s[2], s[3] - s[1]),
        (d[0] - minus, d[2] - plus),
    ]


def real_idft(pairs):
    (a0, a4), (b_re, b_im), (c_re, c_im), (d_re, d_im) = pairs
    plus, minus = a0 + a4, a0 - a4
    c_re, c_im = c_re + c_re, c_im + c_im
    e = [plus + c_re, minus - c_im, plus - c_re, minus + c_im]
    diff = (b_re - d_re) * math.sqrt(2.0)
    both = (b_im + d_im) * math.sqrt(2.0)
    o = [2.0 * (b_re + d_re), diff - both, 2.0 * (d_im - b_im), -diff - both]
    return [e[i] + o[i] for i in range(4)] + [e[i] - o[i] for i in range(4)]


def turn_by(value, cos, sin):
    re, im = value
    return re * cos + im * sin, im * cos - re * sin


def add(a, b):
    return a[0] + b[0], a[1] + b[1]


def sub(a, b):
    return a[0] - b[0], a[1] - b[1]


def dft4(v):
    s02, d02, s13, d13 = add(v[0], v[2]), sub(v[0], v[2]), add(v[1], v[3]), sub(v[1], v[3])
    return [
        add(s02, s13),
        (d02[0] + d13[1], d02[1] - d13[0]),
        sub(s02, s13),
        (d02[0] - d13[1], d02[1] + d13[0]),
    ]


def idft4(v):
    s02, d02, s13, d13 = add(v[0], v[2]), sub(v[0], v[2]), add(v[1], v[3]), sub(v[1], v[3])
    return [
        add(s02, s13),
        (d02[0] - d13[1], d02[1] + d13[0]),
        sub(s02, s13),
        (d02[0] + d13[1], d02[1] - d13[0]),
    ]


def dft8(v):
    even = dft4([add(v[i], v[i + 4]) for i in range(4)])
    odd = [sub(v[i], v[i + 4]) for i in range(4)]
    odd = [
        odd[0],
        ((odd[1][0] + odd[1][1]) * HALF_ROOT, (odd[1][1] - odd[1][0]) * HALF_ROOT),
        (odd[2][1], -odd[2][0]),
        ((odd[3][1] - odd[3][0]) * HALF_ROOT, -(odd[3][0] + odd[3][1]) * HALF_ROOT),
    ]
    odd = dft4(odd)
    return [part[i] for i in range(4) for part in (even, odd)]


def idft8(v):
    even = idft4(v[0::2])
    odd = idft4(v[1::2])
    odd = [
        odd[0],
        ((odd[1][0] - odd[1][1]) * HALF_ROOT, (odd[1][1] + odd[1][0]) * HALF_ROOT),
        (-odd[2][1], odd[2][0]),
        (-(odd[3][0] + odd[3][1]) * HALF_ROOT, (odd[3][0] - odd[3][1]) * HALF_ROOT),
    ]
    return [add(even[i], odd[i]) for i in range(4)] + [sub(even[i], odd[i]) for i in range(4)]


SIXTEENTH = [(math.cos(math.pi * i / 8), math.sin(math.pi * i / 8)) for i in range(4)]


def first_chip_dft(z):
    low = real_dft([v[0] for v in z])
    turned = [turn_by((z[i][1], -z[i + 4][1]), *SIXTEENTH[i]) for i in range(4)]
    return low + dft4(turned)


def first_chip_idft(pairs):
    low = real_idft(pairs[:4])
    turned = idft4(pairs[4:])
    turned = [turn_by(turned[i], SIXTEENTH[i][0], -SIXTEENTH[i][1]) for i in range(4)]
    high = [2.0 * t[0] for t in turned] + [-2.0 * t[1] for t in turned]
    return list(zip(low, high))


def other_chip_dft(z, twist):
    return dft8([z[0]] + [turn_by(z[j], *twist[j]) for j in range(1, 8)])


def other_chip_idft(pairs, twist):
    z = idft8(pairs)
    return [z[0]] + [turn_by(z[j], twist[j][0], -twist[j][1]) for j in range(1, 8)]


def kernel(
    bands,
    cut_hbm,
    x_hbm,
    out,
    cut_ref,
    twist_ref,
    y_send,
    y_in,
    x_send,
    x_in,
    r_send,
    r_in,
    o_send,
    o_in,
    gate,
    stage,
    result,
    load_sem,
    ys_sem,
    yr_sem,
    xs_sem,
    xr_sem,
    rs_sem,
    rr_sem,
    os_sem,
    or_sem,
    meet_sem,
    go_sem,
    here_sem,
):
    band = lax.axis_index("lat")
    lon = lax.axis_index("lon")
    y, j = lon // 8, lon % 8
    x, core = j // 2, j % 2
    total_rows = bands * ROWS

    def polar(row):
        return jnp.abs(2 * (band * ROWS + row) + 1 - total_rows) * 5 > 2 * total_rows

    count = sum(polar(row).astype(jnp.int32) for row in range(ROWS))
    first = jnp.where(polar(0), 0, ROWS - count)
    any_polar = count > 0

    def place(there):
        index = (there * count + 7) // 8
        return index, (index < count) & (index * 8 // jnp.maximum(count, 1) == there)

    index, mine = place(y)
    mine = mine & any_polar
    row_here = jnp.minimum(first + index, ROWS - 1)

    def keeper(c):
        return c % 2

    load = pltpu.make_async_copy(x_hbm, out, load_sem.at[0])
    cut_load = pltpu.make_async_copy(cut_hbm, cut_ref, load_sem.at[1])
    load.start()

    late_plane = band == 0
    late = late_plane & (lon == 0)
    late_column = late_plane & (j == 0) & (y != 0)
    late_row = late_plane & (y == 0) & (j != 0)
    x_lag = 2
    r_lag = 4

    barrier = pltpu.get_barrier_semaphore()

    def column_device(there):
        return (band, there * 8 + j)

    def row_device(there):
        return (band, y * 8 + there)

    def signal(sem, device):
        pl.semaphore_signal(sem, inc=1, device_id=device, device_id_type=MESH)

    @pl.when(any_polar & jnp.logical_not(late))
    def _():
        for step in ORDER:
            signal(barrier, column_device((y + step) % 8))

        @pl.when(y == HUB)
        def _():
            for step in range(1, 8):
                signal(barrier, row_device((j + step) % 8))

        @pl.when(late_row)
        def _():
            signal(barrier, row_device(0))

    @pl.when(any_polar & late)
    def _():
        pl.semaphore_wait(barrier, 14)
        for step in ORDER:
            signal(here_sem, column_device((y + step) % 8))
            signal(here_sem, row_device((j + step) % 8))

    cut_load.start()
    load.wait()

    def y_copy(c, there, row, sender):
        return pltpu.make_async_remote_copy(
            src_ref=y_send.at[c, row, pl.ds(0, HALF)],
            dst_ref=y_in.at[c, sender, pl.ds(0, HALF)],
            send_sem=ys_sem,
            recv_sem=yr_sem.at[c],
            device_id=(band, there * 8 + j),
            device_id_type=MESH,
        )

    def x_copy(c, group, sender):
        return pltpu.make_async_remote_copy(
            src_ref=x_send.at[c, group, :, pl.ds(0, HALF)],
            dst_ref=x_in.at[c, sender, :, pl.ds(0, HALF)],
            send_sem=xs_sem.at[(core == keeper(c)).astype(jnp.int32)],
            recv_sem=xr_sem.at[c],
            device_id=(band, y * 8 + group * 2 + keeper(c)),
            device_id_type=MESH,
        )

    def r_copy(c, there, sender):
        return pltpu.make_async_remote_copy(
            src_ref=r_send.at[c, there, :, pl.ds(0, HALF)],
            dst_ref=r_in.at[c, sender, :, pl.ds(0, HALF)],
            send_sem=rs_sem,
            recv_sem=rr_sem.at[c],
            device_id=(band, y * 8 + there),
            device_id_type=MESH,
        )

    def o_copy(c, there, row, sender):
        return pltpu.make_async_remote_copy(
            src_ref=o_send.at[c, there, pl.ds(0, HALF)],
            dst_ref=o_in.at[c, row, pl.ds(0, HALF)],
            send_sem=os_sem,
            recv_sem=or_sem.at[c],
            device_id=(band, there * 8 + j),
            device_id_type=MESH,
        )

    def await_bytes(ref, sem):
        pltpu.make_async_copy(ref, ref, sem).wait()

    def await_parts(ref_of, sem, parts, choices):
        for choice in choices:

            @pl.when(parts == choice)
            def _():
                await_bytes(ref_of(choice), sem)

    rows_used = pl.ds(0, HALF)
    others = count - mine.astype(jnp.int32)

    low_lanes = lax.broadcasted_iota(jnp.int32, (HALF, LANES), 1) < 64

    def swap(value):
        return pltpu.roll(value, 64, 1)

    @pl.when(any_polar)
    def _():
        def pack(b):
            for row in range(ROWS):
                start = b * ROWS + row
                upper = out[pl.ds(start, HALF, stride=BLOCKS * ROWS), :]
                lower = out[pl.ds((HALF - 1) * BLOCKS * ROWS + start, HALF, stride=BLOCKS * ROWS), :]
                y_send[2 * b, row, pl.ds(0, HALF), :] = jnp.where(low_lanes, upper, swap(lower))
                y_send[2 * b + 1, row, pl.ds(0, HALF), :] = jnp.where(low_lanes, swap(upper), lower)

        pack(0)
        fewer = late_column.astype(jnp.int32)

        @pl.when(y == HUB)
        def _():
            pl.semaphore_wait(barrier, 14 - fewer)
            for step in range(1, 8):
                signal(meet_sem, row_device((j + step) % 8))

        @pl.when((y != HUB) & jnp.logical_not(late))
        def _():
            pl.semaphore_wait(barrier, 7 - fewer)

        @pl.loop(0, BLOCKS)
        def _(b):
            for c in (2 * b, 2 * b + 1):
                for step in ORDER:
                    there = (y + step) % 8
                    index_there, holds = place(there)

                    @pl.when(holds & jnp.logical_not(late_column & (there == 0)))
                    def _():
                        y_copy(c, there, first + index_there, y).start()

            @pl.when(b < BLOCKS - 1)
            def _():
                pack(b + 1)

    cut_load.wait()

    def build_gates():
        shape = (PAD, LANES)
        down = lax.broadcasted_iota(jnp.int32, shape, 0)
        across = lax.broadcasted_iota(jnp.int32, shape, 1)

        def longitude(slot):
            return jnp.where(slot < SLOT, slot, slot - SLOT + HALF - 1).astype(F32)

        slot = jnp.where(across < 64, across, jnp.where(across < 64 + SLOT, across - 64 + SLOT, across - 64 - SLOT))
        valid = (slot != HALF) & (slot != SLOT) & (slot < PAD - 1) & (slot >= 0)
        valid = valid & (down < SEG) & ((across < PAD) | ((across >= 64) & (across < 64 + PAD)))
        m_across, m_down = longitude(slot), longitude(down)
        valid_left = (down != HALF) & (down != PAD - 1) & (across < 2 * PAD)
        k_down = 64.0 * down.astype(F32)
        k_across = 64.0 * jnp.where(across < PAD, across, across - PAD).astype(F32)
        upper_rows, used = down < SLOT, across < PAD
        cut = jnp.full(shape, cut_ref[row_here].astype(F32), F32)
        top = cos_sin(cut * (math.pi / NLON))[1]
        rows = lax.broadcasted_iota(jnp.int32, (8, LANES), 0)
        twist_ref[0:8], twist_ref[8:16] = wave_at((rows * x * SEG).astype(F32))

        def ordered(block):
            return jnp.where(used, jnp.where(upper_rows, block, swap(block)), 0.0)

        def circulant(base):
            wave = base + k_down
            cos_right, sin_right = wave_at(wave * m_across)
            folded = jnp.minimum(wave, NLON - wave)
            ratio = top / cos_sin(jnp.maximum(folded, 1.0) * (math.pi / NLON))[1]
            gain = jnp.where(valid, jnp.where(folded <= cut, 1.0, ratio * ratio) * (1.0 / NLON), 0.0)
            right = jnp.concatenate([gain * cos_right, gain * sin_right], axis=0)
            cos_left, sin_left = wave_at((base + k_across) * m_down)
            left = jnp.concatenate([jnp.where(used, cos_left, sin_left), jnp.where(used, sin_left, -cos_left)], axis=0)
            left = jnp.where(jnp.concatenate([valid_left] * 2, axis=0), left, 0.0)[:, : 2 * PAD]
            left_high, right_high = left.astype(BF16), right.astype(BF16)
            left_low = (left - left_high.astype(F32)).astype(BF16)
            right_low = (right - right_high.astype(F32)).astype(BF16)
            dot = functools.partial(jnp.dot, preferred_element_type=F32)
            both = dot(left_high, right_high) + (dot(left_high, right_low) + dot(left_low, right_high))
            return ordered(both[:PAD]), ordered(both[PAD:])

        def put(p, start, block):
            rows = block.shape[0]
            top_part = block.astype(BF16)
            gate[p, pl.ds(start, rows)] = top_part
            gate[p, pl.ds(start + 2 * PAD, rows)] = (block - top_part.astype(F32)).astype(BF16)

        @pl.loop(0, 8, unroll=2)
        def _(p):
            base = x + 8 * p
            for i in range(8):
                base = jnp.where((x == 0) & (p == i), FIRST_WAVES[i], base)
            real, imag = circulant(base.astype(F32))
            put(p, 0, real - pltpu.roll(imag, PAD, 1))
            put(p, PAD, imag + pltpu.roll(real, PAD, 1))

        @pl.when(x == 0)
        def _():
            put(0, PAD, pltpu.roll(circulant(float(FIRST_WAVES[8]))[0], PAD, 1))

    def y_stage(c):
        await_bytes(y_in.at[c, pl.ds(0, 7), rows_used], yr_sem.at[c])
        y_in[c, y, pl.ds(0, HALF)] = y_send[c, row_here, pl.ds(0, HALF)]
        @pl.loop(0, SLOT, step=8)
        def _(m):
            rows = pl.ds(pl.multiple_of(m, 8), 8)
            pairs = real_dft([y_in[c, i, rows] for i in range(8)])
            for group in range(4):
                x_send[c, group, 0, rows], x_send[c, group, 1, rows] = pairs[group]

        @pl.when((c == 0) & (y != HUB) & jnp.logical_not(late))
        def _():
            pl.semaphore_wait(go_sem, 1)

        for group in (3, 2, 1, 0):
            self_held = (x == group) & (core == keeper(c))
            if group == 0:

                @pl.when((c == 0) & late_row)
                def _():
                    pl.semaphore_wait(here_sem, 1)

            @pl.when(self_held)
            def _():
                x_in[c, j, :, pl.ds(0, HALF)] = x_send[c, group, :, pl.ds(0, HALF)]

            @pl.when(jnp.logical_not(self_held))
            def _():
                x_copy(c, group, j).start()

    def x_stage(c):
        await_bytes(x_in.at[c, pl.ds(0, 7), :, rows_used], xr_sem.at[c])
        twist = [(twist_ref[i : i + 1], twist_ref[8 + i : 9 + i]) for i in range(8)]
        eight = lax.broadcasted_iota(jnp.int32, (8, LANES), 0)
        low_eight = lax.broadcasted_iota(jnp.int32, (8, LANES), 1) < 64

        def take(i, part, m):
            return jnp.where(eight < HALF - m, x_in[c, i, part, pl.ds(m, 8)], 0.0)

        def write(pairs, m):
            for p in range(8):
                for part in range(2):
                    stage[p, pl.ds(part * PAD + m, 8)] = pairs[p][part]
                    stage[p, pl.ds(part * PAD + SLOT + m, 8)] = swap(pairs[p][part])

        @pl.when(x == 0)
        def _():
            @pl.loop(0, SLOT, step=8)
            def _(m):
                m = pl.multiple_of(m, 8)
                write(first_chip_dft([(take(i, 0, m), take(i, 1, m)) for i in range(8)]), m)

        @pl.when(x != 0)
        def _():
            @pl.loop(0, SLOT, step=8)
            def _(m):
                m = pl.multiple_of(m, 8)
                write(other_chip_dft([(take(i, 0, m), take(i, 1, m)) for i in range(8)], twist), m)

        for p in range(8):
            value = stage[p]
            big = value.astype(BF16)
            small_part = (value - big.astype(F32)).astype(BF16)
            both = jnp.dot(gate[p, :, 0 : 2 * PAD], big, preferred_element_type=F32)
            rest = jnp.dot(gate[p, 0 : 2 * PAD, 0 : 2 * PAD], small_part, preferred_element_type=F32)
            result[p] = both[0 : 2 * PAD] + both[2 * PAD : 4 * PAD] + rest

        def pairs_at(m):
            def pick(p, part):
                return jnp.where(
                    low_eight, result[p, pl.ds(part * PAD + m, 8)], result[p, pl.ds(part * PAD + SLOT + m, 8)]
                )

            return [(pick(p, 0), pick(p, 1)) for p in range(8)]

        def write_back(z, m):
            for i in range(8):
                r_send[c, i, 0, pl.ds(m, 8)], r_send[c, i, 1, pl.ds(m, 8)] = z[i]

        @pl.when(x == 0)
        def _():
            @pl.loop(0, SLOT, step=8)
            def _(m):
                m = pl.multiple_of(m, 8)
                write_back(first_chip_idft(pairs_at(m)), m)

        @pl.when(x != 0)
        def _():
            @pl.loop(0, SLOT, step=8)
            def _(m):
                m = pl.multiple_of(m, 8)
                write_back(other_chip_idft(pairs_at(m), twist), m)

        for step in (4, 5, 3, 2, 6, 7, 1):
            r_copy(c, (j + step) % 8, x).start()
        r_in[c, x, :, pl.ds(0, HALF)] = r_send[c, j, :, pl.ds(0, HALF)]

    def r_stage(c):
        await_parts(
            lambda n: r_in.at[c, pl.ds(0, n), :, rows_used],
            rr_sem.at[c],
            4 - (core == keeper(c)).astype(jnp.int32),
            (3, 4),
        )

        @pl.loop(0, SLOT, step=8)
        def _(m):
            rows = pl.ds(pl.multiple_of(m, 8), 8)
            values = real_idft([(r_in[c, g, 0, rows], r_in[c, g, 1, rows]) for g in range(4)])
            for i in range(8):
                o_send[c, i, rows] = values[i]
        for step in ORDER:
            o_copy(c, (y + step) % 8, row_here, y).start()
        o_in[c, row_here, pl.ds(0, HALF)] = o_send[c, y, pl.ds(0, HALF)]

    @pl.when(mine)
    def _():
        build_gates()

    @pl.when(any_polar & (y == HUB))
    def _():
        pl.semaphore_wait(meet_sem, 7)
        for step in ORDER:
            there = (y + step) % 8

            @pl.when(jnp.logical_not(late_column & (there == 0)))
            def _():
                signal(go_sem, column_device(there))

    @pl.when(any_polar & late_column)
    def _():
        pl.semaphore_wait(here_sem, 1)

        @pl.when(place(0)[1])
        def _():
            @pl.loop(0, CHUNKS)
            def _(c):
                y_copy(c, 0, first, y).start()

    @pl.when(mine)
    def _():
        @pl.loop(0, CHUNKS + r_lag)
        def _(t):
            @pl.when(t < CHUNKS)
            def _():
                y_stage(t)

            @pl.when((t >= x_lag) & (t < CHUNKS + x_lag) & (core == keeper(t - x_lag)))
            def _():
                x_stage(t - x_lag)

            @pl.when(t >= r_lag)
            def _():
                r_stage(t - r_lag)

    @pl.when(any_polar & jnp.logical_not(mine | late) & (y != HUB))
    def _():
        pl.semaphore_wait(go_sem, 1)

        @pl.when(late_row)
        def _():
            pl.semaphore_wait(here_sem, 1)

    @pl.when(any_polar)
    def _():
        @pl.loop(0, BLOCKS)
        def _(b):
            for c in (2 * b, 2 * b + 1):
                await_parts(lambda n: o_in.at[c, pl.ds(0, n), rows_used], or_sem.at[c], others, range(1, 8))

            def unpack(row):
                left, right = o_in[2 * b, row, pl.ds(0, HALF), :], o_in[2 * b + 1, row, pl.ds(0, HALF), :]
                start = b * ROWS + row
                out[pl.ds(start, HALF, stride=BLOCKS * ROWS), :] = jnp.where(low_lanes, left, swap(right))
                out[pl.ds((HALF - 1) * BLOCKS * ROWS + start, HALF, stride=BLOCKS * ROWS), :] = jnp.where(
                    low_lanes, swap(left), right
                )

            @pl.when(count == ROWS)
            def _():
                for row in range(ROWS):
                    unpack(row)

            @pl.when(count < ROWS)
            def _():
                for row in range(ROWS):
                    pl.when(polar(row))(functools.partial(unpack, row))

        await_parts(lambda n: y_send.at[:, pl.ds(0, n), rows_used], ys_sem, others, range(1, 8))

    @pl.when(mine)
    def _():
        await_bytes(x_send.at[pl.ds(0, CHUNKS // 2), :, :, rows_used], xs_sem.at[0])
        await_bytes(x_send.at[pl.ds(0, CHUNKS // 2), pl.ds(0, 3), :, rows_used], xs_sem.at[1])
        await_bytes(r_send.at[pl.ds(0, CHUNKS // 2), pl.ds(0, 7), :, rows_used], rs_sem)
        await_bytes(o_send.at[:, pl.ds(0, 7), rows_used], os_sem)


def local(bands, fields, cutoff):
    flat = jnp.transpose(fields.reshape(ROWS, SEG, BLOCKS, LANES), (1, 2, 0, 3)).reshape(SEG * BLOCKS * ROWS, LANES)
    vmem, dma = pltpu.VMEM, pltpu.SemaphoreType.DMA
    hbm = pl.BlockSpec(memory_space=pltpu.HBM)
    out = pl.pallas_call(
        functools.partial(kernel, bands),
        out_shape=jax.ShapeDtypeStruct(flat.shape, F32),
        in_specs=[hbm] * 2,
        out_specs=pl.BlockSpec(memory_space=pltpu.VMEM),
        scratch_shapes=[
            pltpu.SMEM((ROWS,), jnp.int32),
            vmem((16, LANES), F32),
            vmem((CHUNKS, 8, SLOT, LANES), F32),
            vmem((CHUNKS, 8, SLOT, LANES), F32),
            vmem((CHUNKS, 4, 2, SLOT, LANES), F32),
            vmem((CHUNKS, 8, 2, SLOT, LANES), F32),
            vmem((CHUNKS, 8, 2, SLOT, LANES), F32),
            vmem((CHUNKS, 4, 2, SLOT, LANES), F32),
            vmem((CHUNKS, 8, SLOT, LANES), F32),
            vmem((CHUNKS, 8, SLOT, LANES), F32),
            vmem((8, 4 * PAD, LANES), BF16),
            vmem((8, 2 * PAD, LANES), F32),
            vmem((8, 2 * PAD, LANES), F32),
            dma((2,)),
            dma,
            dma((CHUNKS,)),
            dma((2,)),
            dma((CHUNKS,)),
            dma,
            dma((CHUNKS,)),
            dma,
            dma((CHUNKS,)),
            pltpu.SemaphoreType.REGULAR,
            pltpu.SemaphoreType.REGULAR,
            pltpu.SemaphoreType.REGULAR,
        ],
        compiler_params=pltpu.CompilerParams(
            collective_id=0, has_side_effects=True, vmem_limit_bytes=54304 * 1024
        ),
    )(cutoff, flat)
    filtered = jnp.transpose(out.reshape(SEG, BLOCKS, ROWS, LANES), (2, 0, 1, 3))
    return filtered.reshape(ROWS, SEG, BLOCKS * LANES)


def solution(mesh):
    return jax.shard_map(
        functools.partial(local, mesh.shape["lat"]),
        mesh=mesh,
        in_specs=(P("lat", "lon", None), P("lat")),
        out_specs=P("lat", "lon", None),
        check_vma=False,
    )
```

```python
import functools
import math

import jax
import jax.numpy as jnp
from jax import lax
from jax.experimental import pallas as pl
from jax.experimental.pallas import tpu as pltpu
from jax.sharding import PartitionSpec as P

MESH = pl.DeviceIdType.MESH
F32 = jnp.float32
BF16 = jnp.bfloat16
NLON = 2880
SEG = 45
PAD = 48
HALF = 23
SLOT = 24
ROWS = 8
LANES = 128
BLOCKS = 3
CHUNKS = 6
ORDER = (4, 3, 5, 2, 6, 1, 7)
HUB = 1
HALF_ROOT = math.sqrt(0.5)


FIRST_WAVES = (0, 8, 16, 24, 4, 20, 36, 52, 32)
COS_TERMS = [(-1) ** i / math.factorial(2 * i) for i in range(11)]
SIN_TERMS = [(-1) ** i / math.factorial(2 * i + 1) for i in range(11)]


def cos_sin(angle):
    square = angle * angle
    cos, sin = COS_TERMS[-1], SIN_TERMS[-1]
    for i in reversed(range(10)):
        cos, sin = cos * square + COS_TERMS[i], sin * square + SIN_TERMS[i]
    return cos, sin * angle


def wave_at(step):
    step = step - NLON * jnp.floor(step * (1.0 / NLON) + 0.5)
    return cos_sin(step * (2.0 * math.pi / NLON))


def real_dft(v):
    s = [v[i] + v[i + 4] for i in range(4)]
    d = [v[i] - v[i + 4] for i in range(4)]
    even, odd = s[0] + s[2], s[1] + s[3]
    minus = (d[1] - d[3]) * HALF_ROOT
    plus = (d[1] + d[3]) * HALF_ROOT
    return [
        (even + odd, even - odd),
        (d[0] + minus, -d[2] - plus),
        (s[0] - s[2], s[3] - s[1]),
        (d[0] - minus, d[2] - plus),
    ]


def real_idft(pairs):
    (a0, a4), (b_re, b_im), (c_re, c_im), (d_re, d_im) = pairs
    plus, minus = a0 + a4, a0 - a4
    c_re, c_im = c_re + c_re, c_im + c_im
    e = [plus + c_re, minus - c_im, plus - c_re, minus + c_im]
    diff = (b_re - d_re) * math.sqrt(2.0)
    both = (b_im + d_im) * math.sqrt(2.0)
    o = [2.0 * (b_re + d_re), diff - both, 2.0 * (d_im - b_im), -diff - both]
    return [e[i] + o[i] for i in range(4)] + [e[i] - o[i] for i in range(4)]


def turn_by(value, cos, sin):
    re, im = value
    return re * cos + im * sin, im * cos - re * sin


def add(a, b):
    return a[0] + b[0], a[1] + b[1]


def sub(a, b):
    return a[0] - b[0], a[1] - b[1]


def dft4(v):
    s02, d02, s13, d13 = add(v[0], v[2]), sub(v[0], v[2]), add(v[1], v[3]), sub(v[1], v[3])
    return [
        add(s02, s13),
        (d02[0] + d13[1], d02[1] - d13[0]),
        sub(s02, s13),
        (d02[0] - d13[1], d02[1] + d13[0]),
    ]


def idft4(v):
    s02, d02, s13, d13 = add(v[0], v[2]), sub(v[0], v[2]), add(v[1], v[3]), sub(v[1], v[3])
    return [
        add(s02, s13),
        (d02[0] - d13[1], d02[1] + d13[0]),
        sub(s02, s13),
        (d02[0] + d13[1], d02[1] - d13[0]),
    ]


def dft8(v):
    even = dft4([add(v[i], v[i + 4]) for i in range(4)])
    odd = [sub(v[i], v[i + 4]) for i in range(4)]
    odd = [
        odd[0],
        ((odd[1][0] + odd[1][1]) * HALF_ROOT, (odd[1][1] - odd[1][0]) * HALF_ROOT),
        (odd[2][1], -odd[2][0]),
        ((odd[3][1] - odd[3][0]) * HALF_ROOT, -(odd[3][0] + odd[3][1]) * HALF_ROOT),
    ]
    odd = dft4(odd)
    return [part[i] for i in range(4) for part in (even, odd)]


def idft8(v):
    even = idft4(v[0::2])
    odd = idft4(v[1::2])
    odd = [
        odd[0],
        ((odd[1][0] - odd[1][1]) * HALF_ROOT, (odd[1][1] + odd[1][0]) * HALF_ROOT),
        (-odd[2][1], odd[2][0]),
        (-(odd[3][0] + odd[3][1]) * HALF_ROOT, (odd[3][0] - odd[3][1]) * HALF_ROOT),
    ]
    return [add(even[i], odd[i]) for i in range(4)] + [sub(even[i], odd[i]) for i in range(4)]


SIXTEENTH = [(math.cos(math.pi * i / 8), math.sin(math.pi * i / 8)) for i in range(4)]


def first_chip_dft(z):
    low = real_dft([v[0] for v in z])
    turned = [turn_by((z[i][1], -z[i + 4][1]), *SIXTEENTH[i]) for i in range(4)]
    return low + dft4(turned)


def first_chip_idft(pairs):
    low = real_idft(pairs[:4])
    turned = idft4(pairs[4:])
    turned = [turn_by(turned[i], SIXTEENTH[i][0], -SIXTEENTH[i][1]) for i in range(4)]
    high = [2.0 * t[0] for t in turned] + [-2.0 * t[1] for t in turned]
    return list(zip(low, high))


def other_chip_dft(z, twist):
    return dft8([z[0]] + [turn_by(z[j], *twist[j]) for j in range(1, 8)])


def other_chip_idft(pairs, twist):
    z = idft8(pairs)
    return [z[0]] + [turn_by(z[j], twist[j][0], -twist[j][1]) for j in range(1, 8)]


def kernel(
    bands,
    cut_hbm,
    x_hbm,
    out,
    cut_ref,
    twist_ref,
    y_send,
    y_in,
    x_send,
    x_in,
    r_send,
    r_in,
    o_send,
    o_in,
    gate,
    stage,
    result,
    load_sem,
    ys_sem,
    yr_sem,
    xs_sem,
    xr_sem,
    rs_sem,
    rr_sem,
    os_sem,
    or_sem,
    meet_sem,
    go_sem,
    here_sem,
    y_relay,
    relay_sem,
    pass_sem,
):
    band = lax.axis_index("lat")
    lon = lax.axis_index("lon")
    y, j = lon // 8, lon % 8
    x, core = j // 2, j % 2
    total_rows = bands * ROWS

    def polar(row):
        return jnp.abs(2 * (band * ROWS + row) + 1 - total_rows) * 5 > 2 * total_rows

    count = sum(polar(row).astype(jnp.int32) for row in range(ROWS))
    first = jnp.where(polar(0), 0, ROWS - count)
    any_polar = count > 0

    def place(there):
        index = (there * count + 7) // 8
        return index, (index < count) & (index * 8 // jnp.maximum(count, 1) == there)

    index, mine = place(y)
    mine = mine & any_polar
    row_here = jnp.minimum(first + index, ROWS - 1)

    def keeper(c):
        return c % 2

    load = pltpu.make_async_copy(x_hbm, out, load_sem.at[0])
    cut_load = pltpu.make_async_copy(cut_hbm, cut_ref, load_sem.at[1])
    load.start()

    late_plane = band == 0
    late = late_plane & (lon == 0)
    late_column = late_plane & (j == 0) & (y != 0)
    late_row = late_plane & (y == 0) & (j != 0)
    relay = late_plane & (lon == 1)
    x_lag = 2
    r_lag = 4

    barrier = pltpu.get_barrier_semaphore()

    def column_device(there):
        return (band, there * 8 + j)

    def row_device(there):
        return (band, y * 8 + there)

    def signal(sem, device):
        pl.semaphore_signal(sem, inc=1, device_id=device, device_id_type=MESH)

    @pl.when(any_polar & jnp.logical_not(late))
    def _():
        for step in ORDER:
            signal(barrier, column_device((y + step) % 8))

        @pl.when(y == HUB)
        def _():
            for step in range(1, 8):
                signal(barrier, row_device((j + step) % 8))

        @pl.when(late_row)
        def _():
            signal(barrier, row_device(0))

        @pl.when(relay)
        def _():
            for step in ORDER:
                signal(barrier, (band, step * 8))

    @pl.when(any_polar & late)
    def _():
        pl.semaphore_wait(barrier, 14)
        for step in ORDER:
            signal(here_sem, column_device((y + step) % 8))
            signal(here_sem, row_device((j + step) % 8))

    cut_load.start()
    load.wait()

    def y_copy(c, there, row, sender):
        return pltpu.make_async_remote_copy(
            src_ref=y_send.at[c, row, pl.ds(0, HALF)],
            dst_ref=y_in.at[c, sender, pl.ds(0, HALF)],
            send_sem=ys_sem,
            recv_sem=yr_sem.at[c],
            device_id=(band, there * 8 + j),
            device_id_type=MESH,
        )

    def relay_copy(c):
        return pltpu.make_async_remote_copy(
            src_ref=y_send.at[c, first, pl.ds(0, HALF)],
            dst_ref=y_relay.at[c, y, pl.ds(0, HALF)],
            send_sem=ys_sem,
            recv_sem=relay_sem.at[c],
            device_id=(band, 1),
            device_id_type=MESH,
        )

    def pass_copy(c):
        return pltpu.make_async_remote_copy(
            src_ref=y_relay.at[c, pl.ds(1, 7), pl.ds(0, HALF)],
            dst_ref=y_in.at[c, pl.ds(1, 7), pl.ds(0, HALF)],
            send_sem=pass_sem,
            recv_sem=yr_sem.at[c],
            device_id=(band, 0),
            device_id_type=MESH,
        )

    def x_copy(c, group, sender):
        return pltpu.make_async_remote_copy(
            src_ref=x_send.at[c, group, :, pl.ds(0, HALF)],
            dst_ref=x_in.at[c, sender, :, pl.ds(0, HALF)],
            send_sem=xs_sem.at[(core == keeper(c)).astype(jnp.int32)],
            recv_sem=xr_sem.at[c],
            device_id=(band, y * 8 + group * 2 + keeper(c)),
            device_id_type=MESH,
        )

    def r_copy(c, there, sender):
        return pltpu.make_async_remote_copy(
            src_ref=r_send.at[c, there, :, pl.ds(0, HALF)],
            dst_ref=r_in.at[c, sender, :, pl.ds(0, HALF)],
            send_sem=rs_sem,
            recv_sem=rr_sem.at[c],
            device_id=(band, y * 8 + there),
            device_id_type=MESH,
        )

    def o_copy(c, there, row, sender):
        return pltpu.make_async_remote_copy(
            src_ref=o_send.at[c, there, pl.ds(0, HALF)],
            dst_ref=o_in.at[c, row, pl.ds(0, HALF)],
            send_sem=os_sem,
            recv_sem=or_sem.at[c],
            device_id=(band, there * 8 + j),
            device_id_type=MESH,
        )

    def await_bytes(ref, sem):
        pltpu.make_async_copy(ref, ref, sem).wait()

    def await_parts(ref_of, sem, parts, choices):
        for choice in choices:

            @pl.when(parts == choice)
            def _():
                await_bytes(ref_of(choice), sem)

    rows_used = pl.ds(0, HALF)
    others = count - mine.astype(jnp.int32)

    low_lanes = lax.broadcasted_iota(jnp.int32, (HALF, LANES), 1) < 64

    def swap(value):
        return pltpu.roll(value, 64, 1)

    @pl.when(any_polar)
    def _():
        def pack(b):
            for row in range(ROWS):
                start = b * ROWS + row
                upper = out[pl.ds(start, HALF, stride=BLOCKS * ROWS), :]
                lower = out[pl.ds((HALF - 1) * BLOCKS * ROWS + start, HALF, stride=BLOCKS * ROWS), :]
                y_send[2 * b, row, pl.ds(0, HALF), :] = jnp.where(low_lanes, upper, swap(lower))
                y_send[2 * b + 1, row, pl.ds(0, HALF), :] = jnp.where(low_lanes, swap(upper), lower)

        pack(0)
        @pl.when(y == HUB)
        def _():
            pl.semaphore_wait(barrier, 14)
            for step in range(1, 8):
                signal(meet_sem, row_device((j + step) % 8))

        @pl.when((y != HUB) & jnp.logical_not(late))
        def _():
            pl.semaphore_wait(barrier, 7)

        @pl.loop(0, BLOCKS)
        def _(b):
            for c in (2 * b, 2 * b + 1):
                for step in ORDER:
                    there = (y + step) % 8
                    index_there, holds = place(there)

                    by_relay = late_column & (there == 0)

                    @pl.when(holds & jnp.logical_not(by_relay))
                    def _():
                        y_copy(c, there, first + index_there, y).start()

                    @pl.when(holds & by_relay)
                    def _():
                        relay_copy(c).start()

            @pl.when(b < BLOCKS - 1)
            def _():
                pack(b + 1)

    cut_load.wait()

    def build_gates():
        shape = (PAD, LANES)
        down = lax.broadcasted_iota(jnp.int32, shape, 0)
        across = lax.broadcasted_iota(jnp.int32, shape, 1)

        def longitude(slot):
            return jnp.where(slot < SLOT, slot, slot - SLOT + HALF - 1).astype(F32)

        slot = jnp.where(across < 64, across, jnp.where(across < 64 + SLOT, across - 64 + SLOT, across - 64 - SLOT))
        valid = (slot != HALF) & (slot != SLOT) & (slot < PAD - 1) & (slot >= 0)
        valid = valid & (down < SEG) & ((across < PAD) | ((across >= 64) & (across < 64 + PAD)))
        m_across, m_down = longitude(slot), longitude(down)
        valid_left = (down != HALF) & (down != PAD - 1) & (across < 2 * PAD)
        k_down = 64.0 * down.astype(F32)
        k_across = 64.0 * jnp.where(across < PAD, across, across - PAD).astype(F32)
        upper_rows, used = down < SLOT, across < PAD
        cut = jnp.full(shape, cut_ref[row_here].astype(F32), F32)
        top = cos_sin(cut * (math.pi / NLON))[1]
        rows = lax.broadcasted_iota(jnp.int32, (8, LANES), 0)
        twist_ref[0:8], twist_ref[8:16] = wave_at((rows * x * SEG).astype(F32))

        def ordered(block):
            return jnp.where(used, jnp.where(upper_rows, block, swap(block)), 0.0)

        def circulant(base):
            wave = base + k_down
            cos_right, sin_right = wave_at(wave * m_across)
            folded = jnp.minimum(wave, NLON - wave)
            ratio = top / cos_sin(jnp.maximum(folded, 1.0) * (math.pi / NLON))[1]
            gain = jnp.where(valid, jnp.where(folded <= cut, 1.0, ratio * ratio) * (1.0 / NLON), 0.0)
            right = jnp.concatenate([gain * cos_right, gain * sin_right], axis=0)
            cos_left, sin_left = wave_at((base + k_across) * m_down)
            left = jnp.concatenate([jnp.where(used, cos_left, sin_left), jnp.where(used, sin_left, -cos_left)], axis=0)
            left = jnp.where(jnp.concatenate([valid_left] * 2, axis=0), left, 0.0)[:, : 2 * PAD]
            left_high, right_high = left.astype(BF16), right.astype(BF16)
            left_low = (left - left_high.astype(F32)).astype(BF16)
            right_low = (right - right_high.astype(F32)).astype(BF16)
            dot = functools.partial(jnp.dot, preferred_element_type=F32)
            both = dot(left_high, right_high) + (dot(left_high, right_low) + dot(left_low, right_high))
            return ordered(both[:PAD]), ordered(both[PAD:])

        def put(p, start, block):
            rows = block.shape[0]
            top_part = block.astype(BF16)
            gate[p, pl.ds(start, rows)] = top_part
            gate[p, pl.ds(start + 2 * PAD, rows)] = (block - top_part.astype(F32)).astype(BF16)

        @pl.loop(0, 8, unroll=2)
        def _(p):
            base = x + 8 * p
            for i in range(8):
                base = jnp.where((x == 0) & (p == i), FIRST_WAVES[i], base)
            real, imag = circulant(base.astype(F32))
            put(p, 0, real - pltpu.roll(imag, PAD, 1))
            put(p, PAD, imag + pltpu.roll(real, PAD, 1))

        @pl.when(x == 0)
        def _():
            put(0, PAD, pltpu.roll(circulant(float(FIRST_WAVES[8]))[0], PAD, 1))

    def y_stage(c):
        await_bytes(y_in.at[c, pl.ds(0, 7), rows_used], yr_sem.at[c])
        y_in[c, y, pl.ds(0, HALF)] = y_send[c, row_here, pl.ds(0, HALF)]
        @pl.loop(0, SLOT, step=8)
        def _(m):
            rows = pl.ds(pl.multiple_of(m, 8), 8)
            pairs = real_dft([y_in[c, i, rows] for i in range(8)])
            for group in range(4):
                x_send[c, group, 0, rows], x_send[c, group, 1, rows] = pairs[group]

        @pl.when((c == 0) & (y != HUB) & jnp.logical_not(late))
        def _():
            pl.semaphore_wait(go_sem, 1)

        for group in (3, 2, 1, 0):
            self_held = (x == group) & (core == keeper(c))
            if group == 0:

                @pl.when((c == 0) & late_row)
                def _():
                    pl.semaphore_wait(here_sem, 1)

            @pl.when(self_held)
            def _():
                x_in[c, j, :, pl.ds(0, HALF)] = x_send[c, group, :, pl.ds(0, HALF)]

            @pl.when(jnp.logical_not(self_held))
            def _():
                x_copy(c, group, j).start()

        @pl.when(relay)
        def _():
            await_bytes(y_relay.at[c, pl.ds(0, 7), rows_used], relay_sem.at[c])
            pass_copy(c).start()

    def x_stage(c):
        await_bytes(x_in.at[c, pl.ds(0, 7), :, rows_used], xr_sem.at[c])
        twist = [(twist_ref[i : i + 1], twist_ref[8 + i : 9 + i]) for i in range(8)]
        eight = lax.broadcasted_iota(jnp.int32, (8, LANES), 0)
        low_eight = lax.broadcasted_iota(jnp.int32, (8, LANES), 1) < 64

        def take(i, part, m):
            return jnp.where(eight < HALF - m, x_in[c, i, part, pl.ds(m, 8)], 0.0)

        def write(pairs, m):
            for p in range(8):
                for part in range(2):
                    stage[p, pl.ds(part * PAD + m, 8)] = pairs[p][part]
                    stage[p, pl.ds(part * PAD + SLOT + m, 8)] = swap(pairs[p][part])

        @pl.when(x == 0)
        def _():
            @pl.loop(0, SLOT, step=8)
            def _(m):
                m = pl.multiple_of(m, 8)
                write(first_chip_dft([(take(i, 0, m), take(i, 1, m)) for i in range(8)]), m)

        @pl.when(x != 0)
        def _():
            @pl.loop(0, SLOT, step=8)
            def _(m):
                m = pl.multiple_of(m, 8)
                write(other_chip_dft([(take(i, 0, m), take(i, 1, m)) for i in range(8)], twist), m)

        for p in range(8):
            value = stage[p]
            big = value.astype(BF16)
            small_part = (value - big.astype(F32)).astype(BF16)
            both = jnp.dot(gate[p, :, 0 : 2 * PAD], big, preferred_element_type=F32)
            rest = jnp.dot(gate[p, 0 : 2 * PAD, 0 : 2 * PAD], small_part, preferred_element_type=F32)
            result[p] = both[0 : 2 * PAD] + both[2 * PAD : 4 * PAD] + rest

        def pairs_at(m):
            def pick(p, part):
                return jnp.where(
                    low_eight, result[p, pl.ds(part * PAD + m, 8)], result[p, pl.ds(part * PAD + SLOT + m, 8)]
                )

            return [(pick(p, 0), pick(p, 1)) for p in range(8)]

        def write_back(z, m):
            for i in range(8):
                r_send[c, i, 0, pl.ds(m, 8)], r_send[c, i, 1, pl.ds(m, 8)] = z[i]

        @pl.when(x == 0)
        def _():
            @pl.loop(0, SLOT, step=8)
            def _(m):
                m = pl.multiple_of(m, 8)
                write_back(first_chip_idft(pairs_at(m)), m)

        @pl.when(x != 0)
        def _():
            @pl.loop(0, SLOT, step=8)
            def _(m):
                m = pl.multiple_of(m, 8)
                write_back(other_chip_idft(pairs_at(m), twist), m)

        for step in (4, 5, 3, 2, 6, 7, 1):
            r_copy(c, (j + step) % 8, x).start()
        r_in[c, x, :, pl.ds(0, HALF)] = r_send[c, j, :, pl.ds(0, HALF)]

    def r_stage(c):
        await_parts(
            lambda n: r_in.at[c, pl.ds(0, n), :, rows_used],
            rr_sem.at[c],
            4 - (core == keeper(c)).astype(jnp.int32),
            (3, 4),
        )

        @pl.loop(0, SLOT, step=8)
        def _(m):
            rows = pl.ds(pl.multiple_of(m, 8), 8)
            values = real_idft([(r_in[c, g, 0, rows], r_in[c, g, 1, rows]) for g in range(4)])
            for i in range(8):
                o_send[c, i, rows] = values[i]
        @pl.when((c == 0) & late_column)
        def _():
            pl.semaphore_wait(here_sem, 1)

        for step in ORDER:
            o_copy(c, (y + step) % 8, row_here, y).start()
        o_in[c, row_here, pl.ds(0, HALF)] = o_send[c, y, pl.ds(0, HALF)]

    @pl.when(any_polar & (y == HUB))
    def _():
        pl.semaphore_wait(meet_sem, 7)
        for step in ORDER:
            there = (y + step) % 8

            @pl.when(jnp.logical_not(late_column & (there == 0)))
            def _():
                signal(go_sem, column_device(there))

    @pl.when(mine)
    def _():
        build_gates()

    @pl.when(mine)
    def _():
        @pl.loop(0, CHUNKS + r_lag)
        def _(t):
            @pl.when(t < CHUNKS)
            def _():
                y_stage(t)

            @pl.when((t >= x_lag) & (t < CHUNKS + x_lag) & (core == keeper(t - x_lag)))
            def _():
                x_stage(t - x_lag)

            @pl.when(t >= r_lag)
            def _():
                r_stage(t - r_lag)

    @pl.when(any_polar & jnp.logical_not(mine | late) & (y != HUB))
    def _():
        pl.semaphore_wait(go_sem, 1)

        @pl.when(late_row | late_column)
        def _():
            pl.semaphore_wait(here_sem, 1)

    @pl.when(any_polar)
    def _():
        @pl.loop(0, BLOCKS)
        def _(b):
            for c in (2 * b, 2 * b + 1):
                await_parts(lambda n: o_in.at[c, pl.ds(0, n), rows_used], or_sem.at[c], others, range(1, 8))

            def unpack(row):
                left, right = o_in[2 * b, row, pl.ds(0, HALF), :], o_in[2 * b + 1, row, pl.ds(0, HALF), :]
                start = b * ROWS + row
                out[pl.ds(start, HALF, stride=BLOCKS * ROWS), :] = jnp.where(low_lanes, left, swap(right))
                out[pl.ds((HALF - 1) * BLOCKS * ROWS + start, HALF, stride=BLOCKS * ROWS), :] = jnp.where(
                    low_lanes, swap(left), right
                )

            @pl.when(count == ROWS)
            def _():
                for row in range(ROWS):
                    unpack(row)

            @pl.when(count < ROWS)
            def _():
                for row in range(ROWS):
                    pl.when(polar(row))(functools.partial(unpack, row))

        await_parts(lambda n: y_send.at[:, pl.ds(0, n), rows_used], ys_sem, others, range(1, 8))

    @pl.when(mine)
    def _():
        await_bytes(x_send.at[pl.ds(0, CHUNKS // 2), :, :, rows_used], xs_sem.at[0])
        await_bytes(x_send.at[pl.ds(0, CHUNKS // 2), pl.ds(0, 3), :, rows_used], xs_sem.at[1])
        await_bytes(r_send.at[pl.ds(0, CHUNKS // 2), pl.ds(0, 7), :, rows_used], rs_sem)
        await_bytes(o_send.at[:, pl.ds(0, 7), rows_used], os_sem)

        @pl.when(relay)
        def _():
            await_bytes(y_relay.at[:, pl.ds(0, 7), rows_used], pass_sem)


def local(bands, fields, cutoff):
    flat = jnp.transpose(fields.reshape(ROWS, SEG, BLOCKS, LANES), (1, 2, 0, 3)).reshape(SEG * BLOCKS * ROWS, LANES)
    vmem, dma = pltpu.VMEM, pltpu.SemaphoreType.DMA
    hbm = pl.BlockSpec(memory_space=pltpu.HBM)
    out = pl.pallas_call(
        functools.partial(kernel, bands),
        out_shape=jax.ShapeDtypeStruct(flat.shape, F32),
        in_specs=[hbm] * 2,
        out_specs=pl.BlockSpec(memory_space=pltpu.VMEM),
        scratch_shapes=[
            pltpu.SMEM((ROWS,), jnp.int32),
            vmem((16, LANES), F32),
            vmem((CHUNKS, 8, SLOT, LANES), F32),
            vmem((CHUNKS, 8, SLOT, LANES), F32),
            vmem((CHUNKS, 4, 2, SLOT, LANES), F32),
            vmem((CHUNKS, 8, 2, SLOT, LANES), F32),
            vmem((CHUNKS, 8, 2, SLOT, LANES), F32),
            vmem((CHUNKS, 4, 2, SLOT, LANES), F32),
            vmem((CHUNKS, 8, SLOT, LANES), F32),
            vmem((CHUNKS, 8, SLOT, LANES), F32),
            vmem((8, 4 * PAD, LANES), BF16),
            vmem((8, 2 * PAD, LANES), F32),
            vmem((8, 2 * PAD, LANES), F32),
            dma((2,)),
            dma,
            dma((CHUNKS,)),
            dma((2,)),
            dma((CHUNKS,)),
            dma,
            dma((CHUNKS,)),
            dma,
            dma((CHUNKS,)),
            pltpu.SemaphoreType.REGULAR,
            pltpu.SemaphoreType.REGULAR,
            pltpu.SemaphoreType.REGULAR,
            vmem((CHUNKS, 8, SLOT, LANES), F32),
            dma((CHUNKS,)),
            dma,
        ],
        compiler_params=pltpu.CompilerParams(
            collective_id=0, has_side_effects=True, vmem_limit_bytes=54304 * 1024
        ),
    )(cutoff, flat)
    filtered = jnp.transpose(out.reshape(SEG, BLOCKS, ROWS, LANES), (2, 0, 1, 3))
    return filtered.reshape(ROWS, SEG, BLOCKS * LANES)


def solution(mesh):
    return jax.shard_map(
        functools.partial(local, mesh.shape["lat"]),
        mesh=mesh,
        in_specs=(P("lat", "lon", None), P("lat")),
        out_specs=P("lat", "lon", None),
        check_vma=False,
    )
```

```python
import functools
import math

import jax
import jax.numpy as jnp
from jax import lax
from jax.experimental import pallas as pl
from jax.experimental.pallas import tpu as pltpu
from jax.sharding import PartitionSpec as P

MESH = pl.DeviceIdType.MESH
F32 = jnp.float32
BF16 = jnp.bfloat16
NLON = 2880
SEG = 45
PAD = 48
HALF = 23
SLOT = 24
ROWS = 8
LANES = 128
BLOCKS = 3
CHUNKS = 6
ORDER = (4, 3, 5, 2, 6, 1, 7)
HUB = 1
HALF_ROOT = math.sqrt(0.5)


FIRST_WAVES = (0, 8, 16, 24, 4, 20, 36, 52, 32)
COS_TERMS = [(-1) ** i / math.factorial(2 * i) for i in range(11)]
SIN_TERMS = [(-1) ** i / math.factorial(2 * i + 1) for i in range(11)]


def cos_sin(angle):
    square = angle * angle
    cos, sin = COS_TERMS[-1], SIN_TERMS[-1]
    for i in reversed(range(10)):
        cos, sin = cos * square + COS_TERMS[i], sin * square + SIN_TERMS[i]
    return cos, sin * angle


def wave_at(step):
    step = step - NLON * jnp.floor(step * (1.0 / NLON) + 0.5)
    return cos_sin(step * (2.0 * math.pi / NLON))


def real_dft(v):
    s = [v[i] + v[i + 4] for i in range(4)]
    d = [v[i] - v[i + 4] for i in range(4)]
    even, odd = s[0] + s[2], s[1] + s[3]
    minus = (d[1] - d[3]) * HALF_ROOT
    plus = (d[1] + d[3]) * HALF_ROOT
    return [
        (even + odd, even - odd),
        (d[0] + minus, -d[2] - plus),
        (s[0] - s[2], s[3] - s[1]),
        (d[0] - minus, d[2] - plus),
    ]


def real_idft(pairs):
    (a0, a4), (b_re, b_im), (c_re, c_im), (d_re, d_im) = pairs
    plus, minus = a0 + a4, a0 - a4
    c_re, c_im = c_re + c_re, c_im + c_im
    e = [plus + c_re, minus - c_im, plus - c_re, minus + c_im]
    diff = (b_re - d_re) * math.sqrt(2.0)
    both = (b_im + d_im) * math.sqrt(2.0)
    o = [2.0 * (b_re + d_re), diff - both, 2.0 * (d_im - b_im), -diff - both]
    return [e[i] + o[i] for i in range(4)] + [e[i] - o[i] for i in range(4)]


def turn_by(value, cos, sin):
    re, im = value
    return re * cos + im * sin, im * cos - re * sin


def add(a, b):
    return a[0] + b[0], a[1] + b[1]


def sub(a, b):
    return a[0] - b[0], a[1] - b[1]


def dft4(v):
    s02, d02, s13, d13 = add(v[0], v[2]), sub(v[0], v[2]), add(v[1], v[3]), sub(v[1], v[3])
    return [
        add(s02, s13),
        (d02[0] + d13[1], d02[1] - d13[0]),
        sub(s02, s13),
        (d02[0] - d13[1], d02[1] + d13[0]),
    ]


def idft4(v):
    s02, d02, s13, d13 = add(v[0], v[2]), sub(v[0], v[2]), add(v[1], v[3]), sub(v[1], v[3])
    return [
        add(s02, s13),
        (d02[0] - d13[1], d02[1] + d13[0]),
        sub(s02, s13),
        (d02[0] + d13[1], d02[1] - d13[0]),
    ]


def dft8(v):
    even = dft4([add(v[i], v[i + 4]) for i in range(4)])
    odd = [sub(v[i], v[i + 4]) for i in range(4)]
    odd = [
        odd[0],
        ((odd[1][0] + odd[1][1]) * HALF_ROOT, (odd[1][1] - odd[1][0]) * HALF_ROOT),
        (odd[2][1], -odd[2][0]),
        ((odd[3][1] - odd[3][0]) * HALF_ROOT, -(odd[3][0] + odd[3][1]) * HALF_ROOT),
    ]
    odd = dft4(odd)
    return [part[i] for i in range(4) for part in (even, odd)]


def idft8(v):
    even = idft4(v[0::2])
    odd = idft4(v[1::2])
    odd = [
        odd[0],
        ((odd[1][0] - odd[1][1]) * HALF_ROOT, (odd[1][1] + odd[1][0]) * HALF_ROOT),
        (-odd[2][1], odd[2][0]),
        (-(odd[3][0] + odd[3][1]) * HALF_ROOT, (odd[3][0] - odd[3][1]) * HALF_ROOT),
    ]
    return [add(even[i], odd[i]) for i in range(4)] + [sub(even[i], odd[i]) for i in range(4)]


SIXTEENTH = [(math.cos(math.pi * i / 8), math.sin(math.pi * i / 8)) for i in range(4)]


def first_chip_dft(z):
    low = real_dft([v[0] for v in z])
    turned = [turn_by((z[i][1], -z[i + 4][1]), *SIXTEENTH[i]) for i in range(4)]
    return low + dft4(turned)


def first_chip_idft(pairs):
    low = real_idft(pairs[:4])
    turned = idft4(pairs[4:])
    turned = [turn_by(turned[i], SIXTEENTH[i][0], -SIXTEENTH[i][1]) for i in range(4)]
    high = [2.0 * t[0] for t in turned] + [-2.0 * t[1] for t in turned]
    return list(zip(low, high))


def other_chip_dft(z, twist):
    return dft8([z[0]] + [turn_by(z[j], *twist[j]) for j in range(1, 8)])


def other_chip_idft(pairs, twist):
    z = idft8(pairs)
    return [z[0]] + [turn_by(z[j], twist[j][0], -twist[j][1]) for j in range(1, 8)]


def kernel(
    bands,
    cut_hbm,
    x_hbm,
    out,
    cut_ref,
    twist_ref,
    y_send,
    y_in,
    x_send,
    x_in,
    r_send,
    r_in,
    o_send,
    o_in,
    gate,
    stage,
    result,
    load_sem,
    ys_sem,
    yr_sem,
    xs_sem,
    xr_sem,
    rs_sem,
    rr_sem,
    os_sem,
    or_sem,
    meet_sem,
    go_sem,
    here_sem,
    y_relay,
    relay_sem,
    pass_sem,
):
    band = lax.axis_index("lat")
    lon = lax.axis_index("lon")
    y, j = lon // 8, lon % 8
    x, core = j // 2, j % 2
    total_rows = bands * ROWS

    def polar(row):
        return jnp.abs(2 * (band * ROWS + row) + 1 - total_rows) * 5 > 2 * total_rows

    count = sum(polar(row).astype(jnp.int32) for row in range(ROWS))
    first = jnp.where(polar(0), 0, ROWS - count)
    any_polar = count > 0

    def place(there):
        index = (there * count + 7) // 8
        return index, (index < count) & (index * 8 // jnp.maximum(count, 1) == there)

    index, mine = place(y)
    mine = mine & any_polar
    row_here = jnp.minimum(first + index, ROWS - 1)

    def keeper(c):
        return c % 2

    load = pltpu.make_async_copy(x_hbm, out, load_sem.at[0])
    cut_load = pltpu.make_async_copy(cut_hbm, cut_ref, load_sem.at[1])
    load.start()

    late_plane = band == 0
    late = late_plane & (lon == 0)
    late_column = late_plane & (j == 0) & (y != 0)
    late_row = late_plane & (y == 0) & (j != 0)
    relay = late_plane & (lon == 1)
    x_lag = 2
    r_lag = 4

    barrier = pltpu.get_barrier_semaphore()

    def column_device(there):
        return (band, there * 8 + j)

    def row_device(there):
        return (band, y * 8 + there)

    def signal(sem, device):
        pl.semaphore_signal(sem, inc=1, device_id=device, device_id_type=MESH)

    @pl.when(any_polar & jnp.logical_not(late))
    def _():
        for step in ORDER:
            signal(barrier, column_device((y + step) % 8))

        @pl.when(y == HUB)
        def _():
            for step in range(1, 8):
                signal(barrier, row_device((j + step) % 8))

        @pl.when(late_row)
        def _():
            signal(barrier, row_device(0))

        @pl.when(relay)
        def _():
            for step in ORDER:
                signal(barrier, (band, step * 8))

    @pl.when(any_polar & late)
    def _():
        pl.semaphore_wait(barrier, 14)
        for step in ORDER:
            signal(here_sem, column_device((y + step) % 8))
            signal(here_sem, row_device((j + step) % 8))

    cut_load.start()
    load.wait()

    def y_copy(c, there, row, sender):
        return pltpu.make_async_remote_copy(
            src_ref=y_send.at[c, row, pl.ds(0, HALF)],
            dst_ref=y_in.at[c, sender, pl.ds(0, HALF)],
            send_sem=ys_sem,
            recv_sem=yr_sem.at[c],
            device_id=(band, there * 8 + j),
            device_id_type=MESH,
        )

    def relay_copy(c):
        return pltpu.make_async_remote_copy(
            src_ref=y_send.at[c, first, pl.ds(0, HALF)],
            dst_ref=y_relay.at[c, y, pl.ds(0, HALF)],
            send_sem=ys_sem,
            recv_sem=relay_sem.at[c],
            device_id=(band, 1),
            device_id_type=MESH,
        )

    def pass_copy(c):
        return pltpu.make_async_remote_copy(
            src_ref=y_relay.at[c, pl.ds(1, 7), pl.ds(0, HALF)],
            dst_ref=y_in.at[c, pl.ds(1, 7), pl.ds(0, HALF)],
            send_sem=pass_sem,
            recv_sem=yr_sem.at[c],
            device_id=(band, 0),
            device_id_type=MESH,
        )

    def x_copy(c, group, sender):
        return pltpu.make_async_remote_copy(
            src_ref=x_send.at[c, group, :, pl.ds(0, HALF)],
            dst_ref=x_in.at[c, sender, :, pl.ds(0, HALF)],
            send_sem=xs_sem.at[(core == keeper(c)).astype(jnp.int32)],
            recv_sem=xr_sem.at[c],
            device_id=(band, y * 8 + group * 2 + keeper(c)),
            device_id_type=MESH,
        )

    def r_copy(c, there, sender):
        return pltpu.make_async_remote_copy(
            src_ref=r_send.at[c, there, :, pl.ds(0, HALF)],
            dst_ref=r_in.at[c, sender, :, pl.ds(0, HALF)],
            send_sem=rs_sem,
            recv_sem=rr_sem.at[c],
            device_id=(band, y * 8 + there),
            device_id_type=MESH,
        )

    def o_copy(c, there, row, sender):
        return pltpu.make_async_remote_copy(
            src_ref=o_send.at[c, there, pl.ds(0, HALF)],
            dst_ref=o_in.at[c, row, pl.ds(0, HALF)],
            send_sem=os_sem,
            recv_sem=or_sem.at[c],
            device_id=(band, there * 8 + j),
            device_id_type=MESH,
        )

    def await_bytes(ref, sem):
        pltpu.make_async_copy(ref, ref, sem).wait()

    def await_parts(ref_of, sem, parts, choices):
        for choice in choices:

            @pl.when(parts == choice)
            def _():
                await_bytes(ref_of(choice), sem)

    rows_used = pl.ds(0, HALF)
    others = count - mine.astype(jnp.int32)

    low_lanes = lax.broadcasted_iota(jnp.int32, (HALF, LANES), 1) < 64

    def swap(value):
        return pltpu.roll(value, 64, 1)

    @pl.when(any_polar)
    def _():
        def pack(b):
            for row in range(ROWS):
                start = b * ROWS + row
                upper = out[pl.ds(start, HALF, stride=BLOCKS * ROWS), :]
                lower = out[pl.ds((HALF - 1) * BLOCKS * ROWS + start, HALF, stride=BLOCKS * ROWS), :]
                y_send[2 * b, row, pl.ds(0, HALF), :] = jnp.where(low_lanes, upper, swap(lower))
                y_send[2 * b + 1, row, pl.ds(0, HALF), :] = jnp.where(low_lanes, swap(upper), lower)

        pack(0)
        @pl.when(y == HUB)
        def _():
            pl.semaphore_wait(barrier, 14)
            for step in range(1, 8):
                signal(meet_sem, row_device((j + step) % 8))

        @pl.when((y != HUB) & jnp.logical_not(late))
        def _():
            pl.semaphore_wait(barrier, 7)

        @pl.loop(0, BLOCKS)
        def _(b):
            for c in (2 * b, 2 * b + 1):
                for step in ORDER:
                    there = (y + step) % 8
                    index_there, holds = place(there)

                    by_relay = late_column & (there == 0)

                    @pl.when(holds & jnp.logical_not(by_relay))
                    def _():
                        y_copy(c, there, first + index_there, y).start()

                    @pl.when(holds & by_relay)
                    def _():
                        relay_copy(c).start()

            @pl.when(b < BLOCKS - 1)
            def _():
                pack(b + 1)

    cut_load.wait()

    def build_gates():
        shape = (PAD, LANES)
        down = lax.broadcasted_iota(jnp.int32, shape, 0)
        across = lax.broadcasted_iota(jnp.int32, shape, 1)

        def longitude(slot):
            return jnp.where(slot < SLOT, slot, slot - SLOT + HALF - 1).astype(F32)

        slot = jnp.where(across < 64, across, jnp.where(across < 64 + SLOT, across - 64 + SLOT, across - 64 - SLOT))
        valid = (slot != HALF) & (slot != SLOT) & (slot < PAD - 1) & (slot >= 0)
        valid = valid & (down < SEG) & ((across < PAD) | ((across >= 64) & (across < 64 + PAD)))
        m_across, m_down = longitude(slot), longitude(down)
        valid_left = (down != HALF) & (down != PAD - 1) & (across < 2 * PAD)
        k_down = 64.0 * down.astype(F32)
        k_across = 64.0 * jnp.where(across < PAD, across, across - PAD).astype(F32)
        upper_rows, used = down < SLOT, across < PAD
        cut = jnp.full(shape, cut_ref[row_here].astype(F32), F32)
        top = cos_sin(cut * (math.pi / NLON))[1]
        rows = lax.broadcasted_iota(jnp.int32, (8, LANES), 0)
        twist_ref[0:8], twist_ref[8:16] = wave_at((rows * x * SEG).astype(F32))

        def ordered(block):
            return jnp.where(used, jnp.where(upper_rows, block, swap(block)), 0.0)

        def circulant(base):
            wave = base + k_down
            cos_right, sin_right = wave_at(wave * m_across)
            folded = jnp.minimum(wave, NLON - wave)
            ratio = top / cos_sin(jnp.maximum(folded, 1.0) * (math.pi / NLON))[1]
            gain = jnp.where(valid, jnp.where(folded <= cut, 1.0, ratio * ratio) * (1.0 / NLON), 0.0)
            right = jnp.concatenate([gain * cos_right, gain * sin_right], axis=0)
            cos_left, sin_left = wave_at((base + k_across) * m_down)
            left = jnp.concatenate([jnp.where(used, cos_left, sin_left), jnp.where(used, sin_left, -cos_left)], axis=0)
            left = jnp.where(jnp.concatenate([valid_left] * 2, axis=0), left, 0.0)[:, : 2 * PAD]
            left_high, right_high = left.astype(BF16), right.astype(BF16)
            left_low = (left - left_high.astype(F32)).astype(BF16)
            right_low = (right - right_high.astype(F32)).astype(BF16)
            dot = functools.partial(jnp.dot, preferred_element_type=F32)
            both = dot(left_high, right_high) + (dot(left_high, right_low) + dot(left_low, right_high))
            return ordered(both[:PAD]), ordered(both[PAD:])

        def put(p, start, block):
            rows = block.shape[0]
            top_part = block.astype(BF16)
            gate[p, pl.ds(start, rows)] = top_part
            gate[p, pl.ds(start + 2 * PAD, rows)] = (block - top_part.astype(F32)).astype(BF16)

        @pl.loop(0, 8, unroll=2)
        def _(p):
            base = x + 8 * p
            for i in range(8):
                base = jnp.where((x == 0) & (p == i), FIRST_WAVES[i], base)
            real, imag = circulant(base.astype(F32))
            put(p, 0, real - pltpu.roll(imag, PAD, 1))
            put(p, PAD, imag + pltpu.roll(real, PAD, 1))

        @pl.when(x == 0)
        def _():
            put(0, PAD, pltpu.roll(circulant(float(FIRST_WAVES[8]))[0], PAD, 1))

    def y_stage(c):
        await_bytes(y_in.at[c, pl.ds(0, 7), rows_used], yr_sem.at[c])
        y_in[c, y, pl.ds(0, HALF)] = y_send[c, row_here, pl.ds(0, HALF)]
        @pl.loop(0, SLOT, step=8, unroll=True)
        def _(m):
            rows = pl.ds(pl.multiple_of(m, 8), 8)
            pairs = real_dft([y_in[c, i, rows] for i in range(8)])
            for group in range(4):
                x_send[c, group, 0, rows], x_send[c, group, 1, rows] = pairs[group]

        @pl.when((c == 0) & (y != HUB) & jnp.logical_not(late))
        def _():
            pl.semaphore_wait(go_sem, 1)

        for group in (3, 2, 1, 0):
            self_held = (x == group) & (core == keeper(c))
            if group == 0:

                @pl.when((c == 0) & late_row)
                def _():
                    pl.semaphore_wait(here_sem, 1)

            @pl.when(self_held)
            def _():
                x_in[c, j, :, pl.ds(0, HALF)] = x_send[c, group, :, pl.ds(0, HALF)]

            @pl.when(jnp.logical_not(self_held))
            def _():
                x_copy(c, group, j).start()

        @pl.when(relay)
        def _():
            await_bytes(y_relay.at[c, pl.ds(0, 7), rows_used], relay_sem.at[c])
            pass_copy(c).start()

    def x_stage(c):
        await_bytes(x_in.at[c, pl.ds(0, 7), :, rows_used], xr_sem.at[c])
        twist = [(twist_ref[i : i + 1], twist_ref[8 + i : 9 + i]) for i in range(8)]
        eight = lax.broadcasted_iota(jnp.int32, (8, LANES), 0)
        low_eight = lax.broadcasted_iota(jnp.int32, (8, LANES), 1) < 64

        def take(i, part, m):
            return jnp.where(eight < HALF - m, x_in[c, i, part, pl.ds(m, 8)], 0.0)

        def write(pairs, m):
            for p in range(8):
                for part in range(2):
                    stage[p, pl.ds(part * PAD + m, 8)] = pairs[p][part]
                    stage[p, pl.ds(part * PAD + SLOT + m, 8)] = swap(pairs[p][part])

        @pl.when(x == 0)
        def _():
            @pl.loop(0, SLOT, step=8, unroll=True)
            def _(m):
                m = pl.multiple_of(m, 8)
                write(first_chip_dft([(take(i, 0, m), take(i, 1, m)) for i in range(8)]), m)

        @pl.when(x != 0)
        def _():
            @pl.loop(0, SLOT, step=8, unroll=True)
            def _(m):
                m = pl.multiple_of(m, 8)
                write(other_chip_dft([(take(i, 0, m), take(i, 1, m)) for i in range(8)], twist), m)

        for p in range(8):
            value = stage[p]
            big = value.astype(BF16)
            small_part = (value - big.astype(F32)).astype(BF16)
            both = jnp.dot(gate[p, :, 0 : 2 * PAD], big, preferred_element_type=F32)
            rest = jnp.dot(gate[p, 0 : 2 * PAD, 0 : 2 * PAD], small_part, preferred_element_type=F32)
            result[p] = both[0 : 2 * PAD] + both[2 * PAD : 4 * PAD] + rest

        def pairs_at(m):
            def pick(p, part):
                return jnp.where(
                    low_eight, result[p, pl.ds(part * PAD + m, 8)], result[p, pl.ds(part * PAD + SLOT + m, 8)]
                )

            return [(pick(p, 0), pick(p, 1)) for p in range(8)]

        def write_back(z, m):
            for i in range(8):
                r_send[c, i, 0, pl.ds(m, 8)], r_send[c, i, 1, pl.ds(m, 8)] = z[i]

        @pl.when(x == 0)
        def _():
            @pl.loop(0, SLOT, step=8, unroll=True)
            def _(m):
                m = pl.multiple_of(m, 8)
                write_back(first_chip_idft(pairs_at(m)), m)

        @pl.when(x != 0)
        def _():
            @pl.loop(0, SLOT, step=8, unroll=True)
            def _(m):
                m = pl.multiple_of(m, 8)
                write_back(other_chip_idft(pairs_at(m), twist), m)

        for step in (4, 5, 3, 2, 6, 7, 1):
            r_copy(c, (j + step) % 8, x).start()
        r_in[c, x, :, pl.ds(0, HALF)] = r_send[c, j, :, pl.ds(0, HALF)]

    def r_stage(c):
        await_parts(
            lambda n: r_in.at[c, pl.ds(0, n), :, rows_used],
            rr_sem.at[c],
            4 - (core == keeper(c)).astype(jnp.int32),
            (3, 4),
        )

        @pl.loop(0, SLOT, step=8, unroll=True)
        def _(m):
            rows = pl.ds(pl.multiple_of(m, 8), 8)
            values = real_idft([(r_in[c, g, 0, rows], r_in[c, g, 1, rows]) for g in range(4)])
            for i in range(8):
                o_send[c, i, rows] = values[i]
        @pl.when((c == 0) & late_column)
        def _():
            pl.semaphore_wait(here_sem, 1)

        for step in ORDER:
            o_copy(c, (y + step) % 8, row_here, y).start()
        o_in[c, row_here, pl.ds(0, HALF)] = o_send[c, y, pl.ds(0, HALF)]

    @pl.when(any_polar & (y == HUB))
    def _():
        pl.semaphore_wait(meet_sem, 7)
        for step in ORDER:
            there = (y + step) % 8

            @pl.when(jnp.logical_not(late_column & (there == 0)))
            def _():
                signal(go_sem, column_device(there))

    @pl.when(mine)
    def _():
        build_gates()

    @pl.when(mine)
    def _():
        @pl.loop(0, CHUNKS + r_lag)
        def _(t):
            @pl.when(t < CHUNKS)
            def _():
                y_stage(t)

            @pl.when((t >= x_lag) & (t < CHUNKS + x_lag) & (core == keeper(t - x_lag)))
            def _():
                x_stage(t - x_lag)

            @pl.when(t >= r_lag)
            def _():
                r_stage(t - r_lag)

    @pl.when(any_polar & jnp.logical_not(mine | late) & (y != HUB))
    def _():
        pl.semaphore_wait(go_sem, 1)

        @pl.when(late_row | late_column)
        def _():
            pl.semaphore_wait(here_sem, 1)

    @pl.when(any_polar)
    def _():
        @pl.loop(0, BLOCKS)
        def _(b):
            for c in (2 * b, 2 * b + 1):
                await_parts(lambda n: o_in.at[c, pl.ds(0, n), rows_used], or_sem.at[c], others, range(1, 8))

            def unpack(row):
                left, right = o_in[2 * b, row, pl.ds(0, HALF), :], o_in[2 * b + 1, row, pl.ds(0, HALF), :]
                start = b * ROWS + row
                out[pl.ds(start, HALF, stride=BLOCKS * ROWS), :] = jnp.where(low_lanes, left, swap(right))
                out[pl.ds((HALF - 1) * BLOCKS * ROWS + start, HALF, stride=BLOCKS * ROWS), :] = jnp.where(
                    low_lanes, swap(left), right
                )

            @pl.when(count == ROWS)
            def _():
                for row in range(ROWS):
                    unpack(row)

            @pl.when(count < ROWS)
            def _():
                for row in range(ROWS):
                    pl.when(polar(row))(functools.partial(unpack, row))

        await_parts(lambda n: y_send.at[:, pl.ds(0, n), rows_used], ys_sem, others, range(1, 8))

    @pl.when(mine)
    def _():
        await_bytes(x_send.at[pl.ds(0, CHUNKS // 2), :, :, rows_used], xs_sem.at[0])
        await_bytes(x_send.at[pl.ds(0, CHUNKS // 2), pl.ds(0, 3), :, rows_used], xs_sem.at[1])
        await_bytes(r_send.at[pl.ds(0, CHUNKS // 2), pl.ds(0, 7), :, rows_used], rs_sem)
        await_bytes(o_send.at[:, pl.ds(0, 7), rows_used], os_sem)

        @pl.when(relay)
        def _():
            await_bytes(y_relay.at[:, pl.ds(0, 7), rows_used], pass_sem)


def local(bands, fields, cutoff):
    flat = jnp.transpose(fields.reshape(ROWS, SEG, BLOCKS, LANES), (1, 2, 0, 3)).reshape(SEG * BLOCKS * ROWS, LANES)
    vmem, dma = pltpu.VMEM, pltpu.SemaphoreType.DMA
    hbm = pl.BlockSpec(memory_space=pltpu.HBM)
    out = pl.pallas_call(
        functools.partial(kernel, bands),
        out_shape=jax.ShapeDtypeStruct(flat.shape, F32),
        in_specs=[hbm] * 2,
        out_specs=pl.BlockSpec(memory_space=pltpu.VMEM),
        scratch_shapes=[
            pltpu.SMEM((ROWS,), jnp.int32),
            vmem((16, LANES), F32),
            vmem((CHUNKS, 8, SLOT, LANES), F32),
            vmem((CHUNKS, 8, SLOT, LANES), F32),
            vmem((CHUNKS, 4, 2, SLOT, LANES), F32),
            vmem((CHUNKS, 8, 2, SLOT, LANES), F32),
            vmem((CHUNKS, 8, 2, SLOT, LANES), F32),
            vmem((CHUNKS, 4, 2, SLOT, LANES), F32),
            vmem((CHUNKS, 8, SLOT, LANES), F32),
            vmem((CHUNKS, 8, SLOT, LANES), F32),
            vmem((8, 4 * PAD, LANES), BF16),
            vmem((8, 2 * PAD, LANES), F32),
            vmem((8, 2 * PAD, LANES), F32),
            dma((2,)),
            dma,
            dma((CHUNKS,)),
            dma((2,)),
            dma((CHUNKS,)),
            dma,
            dma((CHUNKS,)),
            dma,
            dma((CHUNKS,)),
            pltpu.SemaphoreType.REGULAR,
            pltpu.SemaphoreType.REGULAR,
            pltpu.SemaphoreType.REGULAR,
            vmem((CHUNKS, 8, SLOT, LANES), F32),
            dma((CHUNKS,)),
            dma,
        ],
        compiler_params=pltpu.CompilerParams(
            collective_id=0, has_side_effects=True, vmem_limit_bytes=54304 * 1024
        ),
    )(cutoff, flat)
    filtered = jnp.transpose(out.reshape(SEG, BLOCKS, ROWS, LANES), (2, 0, 1, 3))
    return filtered.reshape(ROWS, SEG, BLOCKS * LANES)


def solution(mesh):
    return jax.shard_map(
        functools.partial(local, mesh.shape["lat"]),
        mesh=mesh,
        in_specs=(P("lat", "lon", None), P("lat")),
        out_specs=P("lat", "lon", None),
        check_vma=False,
    )
```
